32 devices in a mesh: tm: 4 (over y, core), lev: 8 (over z, x).
Axes of the slice: x: 2, y: 2, z: 4, core: 2. Of those that a mesh axis runs over, the one named last changes fastest.
Arguments:
- obs_cell: int32 [4, 16384], P('tm'), may hold values from 0 to 65535
- innovation: float32 [4, 64, 16384], P('tm', 'lev'), may hold values from -8 to 8
- tangent: float32 [4, 64, 128, 512], P('tm', 'lev'), may hold values from -0.45 to 0.45
- damping: float32 [4, 64, 128], P('tm'), may hold values from 0.05 to 0.95
- spread: float32 [64, 128], replicated, may hold values from 0.5 to 2
- vertical: float32 [64, 64], replicated, may hold values from -0.75 to 0.75
Outputs:
- gradient: float32 [64, 128, 2, 128], P(None, 'lev', None, 'tm')
The draws below stay inside these ranges and needn't reach their ends.
All inputs are finite; a program needn't handle non-finite values.
Results may differ from the reference program's by a relative error of at most 0.0003.
Values sent between devices are 32-bit elements; how exact they have to be, the bound alone decides.
No kernel may reach another device: no remote copies, remote signals or barrier semaphores. Data moves between devices by JAX's collectives and lax.ppermute only.
A program may use at most 128 MiB of HBM per device.

```python
import math
import jax
import jax.numpy as jnp
from jax import lax

NLAT = 128
NLON = 512
WAVES = 128
LEVELS = 64
OBS = 16384
TIMES = 4


def touch_ends(drawn, stream_key, smallest, top_value):
    index_at = [jax.random.randint(jax.random.fold_in(stream_key, axis), (), 0, length) for axis, length in enumerate(drawn.shape)]
    widest = drawn.shape.index(max(drawn.shape))
    next_to = index_at[:widest] + [(index_at[widest] + 1) % drawn.shape[widest]] + index_at[widest + 1:]
    return drawn.at[tuple(index_at)].set(smallest).at[tuple(next_to)].set(top_value)


def block_scale(own_key, dims, cuts, smallest, largest):
    gain = 1.0
    for position, shards_of in cuts:
        draws = jax.random.uniform(jax.random.fold_in(jax.random.fold_in(own_key, 6), position), (shards_of,), jnp.float32, smallest / len(cuts), largest / len(cuts))
        gain = gain * jnp.repeat(jnp.exp(draws), dims[position] // shards_of).reshape((-1,) + (1,) * (len(dims) - 1 - position))
    return gain


def bell_draw(key, shape, scale, most, shards=(), held_as=jnp.bfloat16):
    loudness = block_scale(key, shape, shards, -0.22, 0.18) if shards else 1.0
    entries = jax.random.normal(key, shape, jnp.float32) * scale * loudness
    return jnp.minimum(jnp.maximum(entries, -most), most).astype(held_as)


def setup_inputs(seed: int = 0) -> dict:
    key_of = jax.random.split(jax.random.key(seed), 7)
    obs_cell = touch_ends(jax.random.randint(key_of[0], (TIMES, OBS), 0, NLAT * NLON), jax.random.fold_in(key_of[0], 1), 0, (NLAT * NLON) - 1).astype(jnp.int32)
    innovation = bell_draw(key_of[1], (TIMES, LEVELS, OBS), 1.5, 8.0, ((0, 4), (1, 8)), jnp.float32)
    tangent = jnp.clip(jax.random.uniform(key_of[2], (TIMES, LEVELS, NLAT, NLON), jnp.float32, -0.45, 0.45) * block_scale(key_of[2], (TIMES, LEVELS, NLAT, NLON), ((0, 4), (1, 8)), -0.4, 0.0), -0.45, 0.45)
    damping = jnp.clip(jnp.exp(math.log(0.95) - 2.944439 * jax.random.uniform(key_of[3], (TIMES, LEVELS, WAVES), jnp.float32) ** block_scale(key_of[3], (TIMES, LEVELS, WAVES), ((0, 4),), -0.2, 0.2)), 0.05, 0.95)
    spread = jnp.clip(jnp.exp(jax.random.uniform(key_of[4], (LEVELS, WAVES), jnp.float32, math.log(0.5), math.log(2.0))), 0.5, 2.0)
    vertical = bell_draw(key_of[5], (LEVELS, LEVELS), LEVELS ** -0.5, 0.75, (), jnp.float32)
    return dict(obs_cell=obs_cell, innovation=innovation, tangent=tangent, damping=damping, spread=spread, vertical=vertical)


PRECISE = lax.Precision.HIGHEST
HALF_GAMMA_LOG = 0.5 * math.log(math.pi) - math.log(2.0)

def fourier_table(lon_count, wave_count):
    longitude = jnp.arange(lon_count, dtype=jnp.int32)[:, None]
    wavenumber = jnp.arange(wave_count, dtype=jnp.int32)[None, :]
    angles = (longitude * wavenumber % lon_count).astype(jnp.float32) * (2.0 * math.pi / lon_count)
    norm_factor = math.sqrt(2.0 / lon_count)
    columns = jnp.stack([jnp.cos(angles), jnp.sin(angles)], axis=2) * norm_factor
    return columns.reshape(lon_count, 2 * wave_count)

def legendre_table(first_wave, wave_block, lat_count, wave_count):
    orders = (first_wave + jnp.arange(wave_block, dtype=jnp.int32)).astype(jnp.float32)[:, None]
    row_index = jnp.arange(lat_count, dtype=jnp.float32)
    latitude = (row_index + 0.5) * (math.pi / lat_count) - 0.5 * math.pi
    sine_lat = jnp.sin(latitude)[None, :]
    cosine = jnp.cos(latitude)[None, :]
    logdiag = -0.5 * math.log(2.0) + 0.5 * (jax.scipy.special.gammaln(orders + 1.5) - HALF_GAMMA_LOG - jax.scipy.special.gammaln(orders + 1.0)) + orders * jnp.log(cosine)
    diagonal = jnp.exp(logdiag)

    def advance(state_pair, degree):
        prev_one, prev_two = state_pair
        upward = jnp.sqrt(jnp.maximum(4.0 * degree * degree - 1.0, 1.0) / jnp.maximum(degree * degree - orders * orders, 1.0))
        lower = degree - 1.0
        downward = jnp.sqrt(jnp.maximum(lower * lower - orders * orders, 0.0) / jnp.maximum(4.0 * lower * lower - 1.0, 1.0))
        recurred = upward * (sine_lat * prev_one - downward * prev_two)
        current = jnp.where(degree < orders, 0.0, jnp.where(degree == orders, diagonal, recurred))
        return ((current, prev_one), current)
    zero_rows = jnp.zeros((wave_block, lat_count), jnp.float32)
    degrees = jnp.arange(wave_count, dtype=jnp.float32)
    _, values = lax.scan(advance, (zero_rows, zero_rows), degrees, unroll=16)
    weight = jnp.sqrt(math.pi / lat_count * cosine)
    return values * weight[None]

def forcing_field(cell_ids, innov_rows, lat_count, lon_count):
    flat_field = jnp.zeros((innov_rows.shape[0], lat_count * lon_count), jnp.float32)
    flat_field = flat_field.at[:, cell_ids].add(innov_rows)
    return flat_field.reshape(innov_rows.shape[0], lat_count, lon_count)

def reference(obs_cell, innovation, tangent, damping, spread, vertical):
    fourier = fourier_table(NLON, WAVES)
    legendre = legendre_table(0, WAVES, NLAT, WAVES)
    adjoint = jnp.zeros((LEVELS, NLAT, NLON), jnp.float32)
    total = jnp.zeros((LEVELS, WAVES, 2, WAVES), jnp.float32)
    for time_step in range(TIMES - 1, -1, -1):
        forced = adjoint + forcing_field(obs_cell[time_step], innovation[time_step], NLAT, NLON)
        coeffs = jnp.einsum('klx,xc->klc', forced, fourier, precision=PRECISE)
        coeffs = coeffs.reshape(LEVELS, NLAT, WAVES, 2)
        spectral = jnp.einsum('klmp,nml->kmpn', coeffs, legendre, precision=PRECISE)
        total = total + spectral
        filtered = spectral * damping[time_step][:, None, None, :]
        synthesized = jnp.einsum('kmpn,nml->klmp', filtered, legendre, precision=PRECISE)
        synthesized = synthesized.reshape(LEVELS, NLAT, 2 * WAVES)
        adjoint = tangent[time_step] * forced + jnp.einsum('klc,xc->klx', synthesized, fourier, precision=PRECISE)
    scaled = total * spread[:, None, None, :]
    return jnp.einsum('kj,kmpn->jmpn', vertical, scaled, precision=PRECISE)
```

```python
import math

import numpy as np

import jax
import jax.numpy as jnp
from jax import lax
from jax.experimental import pallas as pl
from jax.experimental.pallas import tpu as pltpu
from jax.sharding import PartitionSpec as P

PRECISE = lax.Precision.HIGHEST
LANES = 128
SUBLANES = 8
ACCUMULATORS = 8
OBS_BLOCK = 128
WAVE_UNROLL = 16
DEGREE_UNROLL = 16


def vmem():
    return pl.BlockSpec(memory_space=pltpu.VMEM)


def smem():
    return pl.BlockSpec(memory_space=pltpu.SMEM)


def fourier_rows(lon_count, wave_count):
    longitude = np.arange(lon_count)[None, :]
    wavenumber = np.arange(wave_count)[:, None]
    angles = (longitude * wavenumber % lon_count) * (2.0 * math.pi / lon_count)
    rows = np.concatenate([np.cos(angles), np.sin(angles)]) * math.sqrt(2.0 / lon_count)
    rows = rows.astype(np.float32)
    high = rows.astype(jnp.bfloat16)
    low = (rows - high.astype(np.float32)).astype(jnp.bfloat16)
    return high, low


def legendre_seeds(lat_count, wave_count):
    orders = np.arange(wave_count, dtype=np.float64)[:, None]
    degrees = np.arange(wave_count, dtype=np.float64)[None, :]
    latitude = (np.arange(lat_count) + 0.5) * (math.pi / lat_count) - 0.5 * math.pi
    sine = np.sin(latitude)[None, :]
    cosine = np.cos(latitude)[None, :]
    gammas = np.array(
        [
            math.lgamma(order + 1.5) - math.lgamma(1.5) - math.lgamma(order + 1.0)
            for order in range(wave_count)
        ]
    )[:, None]
    diagonal = np.exp(-0.5 * math.log(2.0) + 0.5 * gammas + orders * np.log(cosine))
    diagonal = diagonal * np.sqrt(math.pi / lat_count * cosine)
    upward = np.sqrt(
        np.maximum(4.0 * degrees**2 - 1.0, 1.0) / np.maximum(degrees**2 - orders**2, 1.0)
    )
    lower = degrees - 1.0
    downward = np.sqrt(
        np.maximum(lower**2 - orders**2, 0.0) / np.maximum(4.0 * lower**2 - 1.0, 1.0)
    )
    cast = lambda table: table.astype(np.float32)
    return cast(upward), cast(upward * downward), cast(diagonal), cast(sine)


def split_parts(values):
    high = values.astype(jnp.bfloat16)
    low = (values - high.astype(jnp.float32)).astype(jnp.bfloat16)
    return high, low


def dot(left, right, left_dim, right_dim):
    return lax.dot_general(
        left, right, (((left_dim,), (right_dim,)), ((), ())), preferred_element_type=jnp.float32
    )


def legendre_kernel(upward, downward, diagonal, sine, table, up_now, down_now, values):
    waves, lats = diagonal.shape
    pitch = values.shape[0] // waves
    up_now[...] = upward[...]
    down_now[...] = downward[...]
    order = lax.broadcasted_iota(jnp.int32, (waves, lats), 0)
    sine_rows = jnp.broadcast_to(sine[...], (waves, lats))

    def advance(group, state):
        one, two = state
        up = up_now[...]
        down = down_now[...]
        for step in range(DEGREE_UNROLL):
            degree = group * DEGREE_UNROLL + step
            seed = jnp.where(order == degree, diagonal[...], 0.0)
            current = (up[:, step : step + 1] * sine_rows) * one
            current = current - down[:, step : step + 1] * two + seed
            values[pl.ds(pl.multiple_of(degree * pitch, SUBLANES), waves), :] = current
            one, two = current, one
        up_now[...] = pltpu.roll(up, waves - DEGREE_UNROLL, 1)
        down_now[...] = pltpu.roll(down, waves - DEGREE_UNROLL, 1)
        return one, two

    zeros = jnp.zeros((waves, lats), jnp.float32)
    lax.fori_loop(0, waves // DEGREE_UNROLL, advance, (zeros, zeros))

    def emit(wave, carry):
        rows = values[pl.ds(wave, waves, stride=pitch), :]
        high, low = split_parts(rows)
        table[wave, 0:waves, :] = high
        table[wave, waves : 2 * waves, :] = low
        return carry

    lax.fori_loop(0, waves, emit, 0)


def legendre_table(lat_count, wave_count):
    pitch = wave_count + SUBLANES
    return pl.pallas_call(
        legendre_kernel,
        out_shape=jax.ShapeDtypeStruct((wave_count, 2 * wave_count, lat_count), jnp.bfloat16),
        in_specs=[vmem()] * 4,
        out_specs=vmem(),
        scratch_shapes=[
            pltpu.VMEM((wave_count, wave_count), jnp.float32),
            pltpu.VMEM((wave_count, wave_count), jnp.float32),
            pltpu.VMEM((wave_count * pitch, lat_count), jnp.float32),
        ],
        compiler_params=pltpu.CompilerParams(vmem_limit_bytes=40 * 2**20),
        name="legendre",
    )(*legendre_seeds(lat_count, wave_count))


def scatter_kernel(rows, low_lat, innov, damp, field, data, *sums):
    levels, obs = innov.shape
    lats = field.shape[1] - SUBLANES
    lons = field.shape[2]
    span = LANES // levels
    waves = damp.shape[1]
    for part in sums:
        part[...] = jnp.zeros(part.shape, jnp.float32)
    lane = lax.broadcasted_iota(jnp.int32, (levels, LANES), 1)
    level = lax.broadcasted_iota(jnp.int32, (levels, LANES), 0)
    place = (lane // span == level).astype(jnp.float32)
    one_row = jnp.ones((1, LANES), jnp.float32)
    lane_low = (lax.broadcasted_iota(jnp.int32, (OBS_BLOCK, LANES), 1) % span).astype(jnp.float32)

    def spread_out(block, carry):
        start = pl.multiple_of(block * OBS_BLOCK, OBS_BLOCK)
        values = innov[:, pl.ds(start, OBS_BLOCK)]
        expanded = lax.dot_general(
            values,
            place,
            (((0,), (0,)), ((), ())),
            precision=PRECISE,
            preferred_element_type=jnp.float32,
        )
        low = dot(low_lat[:, pl.ds(start, OBS_BLOCK)], one_row, 0, 0)
        data[pl.ds(start, OBS_BLOCK), :] = jnp.where(low == lane_low, expanded, 0.0)
        return carry

    lax.fori_loop(0, obs // OBS_BLOCK, spread_out, 0)

    def scatter(block, carry):
        start = pl.multiple_of(block * OBS_BLOCK, OBS_BLOCK)
        for step in range(OBS_BLOCK):
            part = sums[step % ACCUMULATORS]
            row = rows[start + step]
            part[pl.ds(row, 1), :] = part[pl.ds(row, 1), :] + data[pl.ds(start + step, 1), :]
        return carry

    lax.fori_loop(0, obs // OBS_BLOCK, scatter, 0)

    for high in range(lats // span):
        for west in range(lons // LANES):
            block = pl.ds(high * lons + west * LANES, LANES)
            total = sums[0][block, :]
            for part in sums[1:]:
                total = total + part[block, :]
            turned = total.T
            for k in range(levels):
                field[k, high * span : (high + 1) * span, west * LANES : (west + 1) * LANES] = (
                    turned[k * span : (k + 1) * span, :]
                )
    field[:, lats:, :] = jnp.zeros((levels, SUBLANES, lons), jnp.float32)
    for k in range(levels):
        field[k, lats : lats + 1, 0:waves] = damp[k : k + 1, :]


def forcing_field(cells, innov, damp, lats, lons):
    levels, obs = innov.shape
    span = LANES // levels
    lat = cells // lons
    rows = (lat // span) * lons + cells % lons
    low_lat = (lat % span).astype(jnp.float32)[None, :]
    sum_rows = lats * lons // span
    return pl.pallas_call(
        scatter_kernel,
        out_shape=jax.ShapeDtypeStruct((levels, lats + SUBLANES, lons), jnp.float32),
        in_specs=[smem(), vmem(), vmem(), vmem()],
        out_specs=vmem(),
        scratch_shapes=[pltpu.VMEM((obs, LANES), jnp.float32)]
        + [pltpu.VMEM((sum_rows, LANES), jnp.float32)] * ACCUMULATORS,
        compiler_params=pltpu.CompilerParams(vmem_limit_bytes=50 * 2**20),
        name="scatter",
    )(rows, low_lat, innov, damp)


def sweep_kernel(forcing, tangent, spread, fourier_high, fourier_low, table, out, forced, work, total):
    waves = table.shape[0]
    lats = table.shape[2]
    times = out.shape[0]
    degree_block = waves // times
    kept = forcing.shape[0] // times
    half = 2 * kept
    rows = max(SUBLANES, 2 * half)
    copies = rows // half
    row = lax.broadcasted_iota(jnp.int32, (rows, waves), 0)
    is_high = (row // half) % 2 == 0
    total[...] = jnp.zeros(total.shape, jnp.float32)

    for time in range(times - 1, -1, -1):
        for k in range(kept):
            here = slice(k * lats, (k + 1) * lats)
            if time == times - 1:
                forced[here, :] = forcing[time * kept + k, 0:lats, :]
            else:
                forced[here, :] = forced[here, :] + forcing[time * kept + k, 0:lats, :]
        high, low = split_parts(forced[...])
        coeffs = dot(fourier_high[...], high, 1, 1)
        coeffs = coeffs + dot(fourier_low[...], high, 1, 1)
        coeffs = coeffs + dot(fourier_high[...], low, 1, 1)
        for k in range(kept):
            for p in range(2):
                piece = coeffs[p * waves : (p + 1) * waves, k * lats : (k + 1) * lats]
                piece_high = piece.astype(jnp.bfloat16).astype(jnp.float32)
                piece_low = piece - piece_high
                for copy in range(copies):
                    at = copy * half + 2 * k + p
                    work[pl.ds(at, waves, stride=rows), :] = (
                        piece_high if copy % 2 == 0 else piece_low
                    )
        damp_rows = []
        for k in range(kept):
            damp_row = forcing[time * kept + k, lats : lats + 1, 0:waves]
            damp_rows += [damp_row, damp_row]
        damp = jnp.concatenate(damp_rows * copies, axis=0)

        def per_wave(group, carry):
            for step in range(WAVE_UNROLL):
                wave = group * WAVE_UNROLL + step
                at = pl.ds(pl.multiple_of(wave * rows, rows), rows)
                both = table[wave]
                product = dot(work[at, :].astype(jnp.bfloat16), both, 1, 1)
                product = product[:, 0:waves] + product[:, waves:]
                spectral = product + pltpu.roll(product, half, 0)
                total[at, :] = total[at, :] + spectral
                if time > 0:
                    filtered = spectral * damp
                    part = filtered.astype(jnp.bfloat16).astype(jnp.float32)
                    part = jnp.where(is_high, part, filtered - part).astype(jnp.bfloat16)
                    result = dot(jnp.concatenate([part, part], axis=1), both, 1, 0)
                    work[at, :] = result + pltpu.roll(result, half, 0)
            return carry

        lax.fori_loop(0, waves // WAVE_UNROLL, per_wave, 0)
        if time > 0:
            for k in range(kept):
                parts = [work[pl.ds(2 * k + p, waves, stride=rows), :].T for p in range(2)]
                synth_high, synth_low = split_parts(jnp.concatenate(parts, axis=1))
                gridded = dot(synth_high, fourier_high[...], 1, 0)
                gridded = gridded + dot(synth_high, fourier_low[...], 1, 0)
                gridded = gridded + dot(synth_low, fourier_high[...], 1, 0)
                here = slice(k * lats, (k + 1) * lats)
                forced[here, :] = tangent[time * kept + k] * forced[here, :] + gridded

    scaled = []
    for k in range(kept):
        for p in range(2):
            scaled.append(
                total[pl.ds(2 * k + p, waves, stride=rows), :] * spread[k : k + 1, :]
            )
    for block in range(times):
        cols = slice(block * degree_block, (block + 1) * degree_block)
        out[block] = jnp.concatenate([piece[:, cols] for piece in scaled], axis=1)


def sweep(forcing, tangent, spread, table, times):
    kept = spread.shape[0]
    lats, lons = tangent.shape[1:]
    waves = table.shape[0]
    rows = max(SUBLANES, 4 * kept)
    high, low = fourier_rows(lons, waves)
    return pl.pallas_call(
        sweep_kernel,
        out_shape=jax.ShapeDtypeStruct((times, waves, 2 * kept * waves // times), jnp.float32),
        in_specs=[vmem()] * 6,
        out_specs=vmem(),
        scratch_shapes=[
            pltpu.VMEM((kept * lats, lons), jnp.float32),
            pltpu.VMEM((waves * rows, lats), jnp.float32),
            pltpu.VMEM((waves * rows, waves), jnp.float32),
        ],
        compiler_params=pltpu.CompilerParams(vmem_limit_bytes=50 * 2**20),
        name="sweep",
    )(forcing, tangent, spread, high, low, table)


def shards(obs_cell, innovation, tangent, damping, spread, vertical):
    sections = lax.axis_size("tm")
    groups = lax.axis_size("lev")
    my_section = lax.axis_index("tm")
    my_group = lax.axis_index("lev")
    lev_dev, lat_rows, lon_cols = tangent.shape[1:]
    wave_count = damping.shape[2]
    repeat = max(1, sections // lev_dev)
    kept = max(1, lev_dev // sections)
    my_first = my_group * lev_dev + (my_section // repeat) * kept

    def exchange(field):
        field = jnp.repeat(field, repeat, axis=0) if repeat > 1 else field
        return lax.all_to_all(field, "tm", split_axis=0, concat_axis=0, tiled=True)

    tangent_mine = exchange(tangent[0])
    damp_here = lax.dynamic_slice_in_dim(damping[0], my_group * lev_dev, lev_dev, 0)
    forcing = forcing_field(obs_cell[0], innovation[0], damp_here, lat_rows, lon_cols)
    forcing_mine = exchange(forcing)
    table = legendre_table(lat_rows, wave_count)
    spread_mine = lax.dynamic_slice_in_dim(spread, my_first, kept, 0)
    blocks = sweep(forcing_mine, tangent_mine, spread_mine, table, sections)

    block_waves = wave_count // groups
    block_degrees = wave_count // sections
    blocks = blocks.reshape(sections * groups, block_waves, 2 * kept * block_degrees)
    owned = lax.all_to_all(blocks, ("tm", "lev"), split_axis=0, concat_axis=0, tiled=True)
    owned = owned.reshape(sections, groups, block_waves, kept, 2, block_degrees)[::repeat]
    mixing = vertical.reshape(groups, sections // repeat, kept, vertical.shape[1])
    return jnp.einsum("gukl,ugmkpn->lmpn", mixing, owned, precision=PRECISE)


def solution(mesh):
    placed = (
        P("tm", None),
        P("tm", "lev", None),
        P("tm", "lev", None, None),
        P("tm", None, None),
        P(),
        P(),
    )
    return jax.shard_map(
        shards, mesh=mesh, in_specs=placed, out_specs=P(None, "lev", None, "tm"), check_vma=False
    )
```

```python
import math

import numpy as np

import jax
import jax.numpy as jnp
from jax import lax
from jax.experimental import pallas as pl
from jax.experimental.pallas import tpu as pltpu
from jax.sharding import PartitionSpec as P

PRECISE = lax.Precision.HIGHEST
LANES = 128
SUBLANES = 8
ACCUMULATORS = 8
OBS_BLOCK = 128
SPREAD_BLOCK = 1024
WAVE_UNROLL = 16
DEGREE_UNROLL = 16


def vmem():
    return pl.BlockSpec(memory_space=pltpu.VMEM)


def smem():
    return pl.BlockSpec(memory_space=pltpu.SMEM)


def fourier_rows(lon_count, wave_count):
    longitude = np.arange(lon_count)[None, :]
    wavenumber = np.arange(wave_count)[:, None]
    angles = (longitude * wavenumber % lon_count) * (2.0 * math.pi / lon_count)
    rows = np.concatenate([np.cos(angles), np.sin(angles)]) * math.sqrt(2.0 / lon_count)
    rows = rows.astype(np.float32)
    high = rows.astype(jnp.bfloat16)
    low = (rows - high.astype(np.float32)).astype(jnp.bfloat16)
    return high, low


def legendre_seeds(lat_count, wave_count):
    orders = np.arange(wave_count, dtype=np.float64)[:, None]
    degrees = np.arange(wave_count, dtype=np.float64)[None, :]
    latitude = (np.arange(lat_count) + 0.5) * (math.pi / lat_count) - 0.5 * math.pi
    sine = np.sin(latitude)[None, :]
    cosine = np.cos(latitude)[None, :]
    gammas = np.array(
        [
            math.lgamma(order + 1.5) - math.lgamma(1.5) - math.lgamma(order + 1.0)
            for order in range(wave_count)
        ]
    )[:, None]
    diagonal = np.exp(-0.5 * math.log(2.0) + 0.5 * gammas + orders * np.log(cosine))
    diagonal = diagonal * np.sqrt(math.pi / lat_count * cosine)
    upward = np.sqrt(
        np.maximum(4.0 * degrees**2 - 1.0, 1.0) / np.maximum(degrees**2 - orders**2, 1.0)
    )
    lower = degrees - 1.0
    downward = np.sqrt(
        np.maximum(lower**2 - orders**2, 0.0) / np.maximum(4.0 * lower**2 - 1.0, 1.0)
    )
    cast = lambda table: table.astype(np.float32)
    return cast(upward), cast(upward * downward), cast(diagonal), cast(sine)


def split_parts(values):
    high = values.astype(jnp.bfloat16)
    low = (values - high.astype(jnp.float32)).astype(jnp.bfloat16)
    return high, low


def dot(left, right, left_dim, right_dim):
    return lax.dot_general(
        left, right, (((left_dim,), (right_dim,)), ((), ())), preferred_element_type=jnp.float32
    )


def legendre_kernel(
    upward, downward, diagonal, sine, analysis, synthesis, up_now, down_now, values
):
    waves, lats = diagonal.shape
    pitch = values.shape[0] // waves
    up_now[...] = upward[...]
    down_now[...] = downward[...]
    order = lax.broadcasted_iota(jnp.int32, (waves, lats), 0)
    sine_rows = jnp.broadcast_to(sine[...], (waves, lats))

    def advance(group, state):
        one, two = state
        up = up_now[...]
        down = down_now[...]
        for step in range(DEGREE_UNROLL):
            degree = group * DEGREE_UNROLL + step
            seed = jnp.where(order == degree, diagonal[...], 0.0)
            current = (up[:, step : step + 1] * sine_rows) * one
            current = current - down[:, step : step + 1] * two + seed
            values[pl.ds(pl.multiple_of(degree * pitch, SUBLANES), waves), :] = current
            one, two = current, one
        up_now[...] = pltpu.roll(up, waves - DEGREE_UNROLL, 1)
        down_now[...] = pltpu.roll(down, waves - DEGREE_UNROLL, 1)
        return one, two

    zeros = jnp.zeros((waves, lats), jnp.float32)
    lax.fori_loop(0, waves // DEGREE_UNROLL, advance, (zeros, zeros))

    def emit(wave, carry):
        rows = values[pl.ds(wave, waves, stride=pitch), :]
        analysis[wave] = jnp.concatenate(split_parts(rows.T), axis=1)
        synthesis[wave] = jnp.concatenate(split_parts(rows), axis=1)
        return carry

    lax.fori_loop(0, waves, emit, 0, unroll=4)


def legendre_tables(lat_count, wave_count):
    pitch = wave_count + SUBLANES
    return pl.pallas_call(
        legendre_kernel,
        out_shape=[
            jax.ShapeDtypeStruct((wave_count, lat_count, 2 * wave_count), jnp.bfloat16),
            jax.ShapeDtypeStruct((wave_count, wave_count, 2 * lat_count), jnp.bfloat16),
        ],
        in_specs=[vmem()] * 4,
        out_specs=[vmem()] * 2,
        scratch_shapes=[
            pltpu.VMEM((wave_count, wave_count), jnp.float32),
            pltpu.VMEM((wave_count, wave_count), jnp.float32),
            pltpu.VMEM((wave_count * pitch, lat_count), jnp.float32),
        ],
        compiler_params=pltpu.CompilerParams(vmem_limit_bytes=40 * 2**20),
        name="legendre",
    )(*legendre_seeds(lat_count, wave_count))


def scatter_kernel(rows, low_lat, innov, damp, field, data, *sums):
    levels, obs = innov.shape
    lats = field.shape[1] - SUBLANES
    lons = field.shape[2]
    span = LANES // levels
    waves = damp.shape[1]
    for part in sums:
        part[...] = jnp.zeros(part.shape, jnp.float32)
    row = lax.broadcasted_iota(jnp.int32, (4 * SUBLANES, 2 * LANES), 0)
    lane = lax.broadcasted_iota(jnp.int32, (4 * SUBLANES, 2 * LANES), 1)
    values_here = (row < 3 * SUBLANES) & (lane < LANES) & (row % SUBLANES == lane // span)
    place = (values_here | ((row == 3 * SUBLANES) & (lane >= LANES))).astype(jnp.bfloat16)
    lane_low = (lax.broadcasted_iota(jnp.int32, (SPREAD_BLOCK, LANES), 1) % span).astype(jnp.float32)

    def spread_out(block, carry):
        start = pl.multiple_of(block * SPREAD_BLOCK, SPREAD_BLOCK)
        rest = innov[:, pl.ds(start, SPREAD_BLOCK)]
        if levels < SUBLANES:
            fill = jnp.zeros((SUBLANES - levels, SPREAD_BLOCK), jnp.float32)
            rest = jnp.concatenate([rest, fill], axis=0)
        parts = []
        for _ in range(3):
            parts.append(rest.astype(jnp.bfloat16).astype(jnp.float32))
            rest = rest - parts[-1]
        low = low_lat[:, pl.ds(start, SPREAD_BLOCK)]
        parts.append(jnp.broadcast_to(low, (SUBLANES, SPREAD_BLOCK)))
        stacked = jnp.concatenate(parts, axis=0).astype(jnp.bfloat16)
        placed = dot(stacked, place, 0, 0)
        data[pl.ds(start, SPREAD_BLOCK), :] = jnp.where(
            placed[:, LANES:] == lane_low, placed[:, :LANES], 0.0
        )
        return carry

    lax.fori_loop(0, obs // SPREAD_BLOCK, spread_out, 0)

    def scatter(block, carry):
        start = pl.multiple_of(block * OBS_BLOCK, OBS_BLOCK)
        for step in range(OBS_BLOCK):
            part = sums[step % ACCUMULATORS]
            row = rows[start + step]
            part[pl.ds(row, 1), :] = part[pl.ds(row, 1), :] + data[pl.ds(start + step, 1), :]
        return carry

    lax.fori_loop(0, obs // OBS_BLOCK, scatter, 0)

    for high in range(lats // span):
        for west in range(lons // LANES):
            block = pl.ds(high * lons + west * LANES, LANES)
            total = sums[0][block, :]
            for part in sums[1:]:
                total = total + part[block, :]
            turned = total.T
            for k in range(levels):
                field[k, high * span : (high + 1) * span, west * LANES : (west + 1) * LANES] = (
                    turned[k * span : (k + 1) * span, :]
                )
    field[:, lats:, :] = jnp.zeros((levels, SUBLANES, lons), jnp.float32)
    for k in range(levels):
        field[k, lats : lats + 1, 0:waves] = damp[k : k + 1, :]


def forcing_field(cells, innov, damp, lats, lons):
    levels, obs = innov.shape
    span = LANES // levels
    lat = cells // lons
    rows = (lat // span) * lons + cells % lons
    low_lat = (lat % span).astype(jnp.float32)[None, :]
    sum_rows = lats * lons // span
    return pl.pallas_call(
        scatter_kernel,
        out_shape=jax.ShapeDtypeStruct((levels, lats + SUBLANES, lons), jnp.float32),
        in_specs=[smem(), vmem(), vmem(), vmem()],
        out_specs=vmem(),
        scratch_shapes=[pltpu.VMEM((obs, LANES), jnp.float32)]
        + [pltpu.VMEM((sum_rows, LANES), jnp.float32)] * ACCUMULATORS,
        compiler_params=pltpu.CompilerParams(vmem_limit_bytes=50 * 2**20),
        name="scatter",
    )(rows, low_lat, innov, damp)


def sweep_kernel(
    forcing,
    tangent,
    spread,
    fourier_high,
    fourier_low,
    analysis,
    synthesis,
    out,
    forced,
    work,
    filtered,
    total,
):
    waves, lats = analysis.shape[:2]
    times = out.shape[0]
    degree_block = waves // times
    kept = forcing.shape[0] // times
    half = 2 * kept
    rows = max(SUBLANES, 2 * half)
    copies = rows // half
    row = lax.broadcasted_iota(jnp.int32, (rows, waves), 0)
    is_high = (row // half) % 2 == 0
    total[...] = jnp.zeros(total.shape, jnp.float32)

    for time in range(times - 1, -1, -1):
        for k in range(kept):
            here = slice(k * lats, (k + 1) * lats)
            if time == times - 1:
                forced[here, :] = forcing[time * kept + k, 0:lats, :]
            else:
                forced[here, :] = forced[here, :] + forcing[time * kept + k, 0:lats, :]
        high, low = split_parts(forced[...])
        coeffs = dot(fourier_high[...], high, 1, 1)
        coeffs = coeffs + dot(fourier_low[...], high, 1, 1)
        coeffs = coeffs + dot(fourier_high[...], low, 1, 1)
        for k in range(kept):
            for p in range(2):
                piece = coeffs[p * waves : (p + 1) * waves, k * lats : (k + 1) * lats]
                piece_high = piece.astype(jnp.bfloat16).astype(jnp.float32)
                piece_low = piece - piece_high
                for copy in range(copies):
                    at = copy * half + 2 * k + p
                    work[pl.ds(at, waves, stride=rows), :] = (
                        piece_high if copy % 2 == 0 else piece_low
                    )
        damp_rows = []
        for k in range(kept):
            damp_row = forcing[time * kept + k, lats : lats + 1, 0:waves]
            damp_rows += [damp_row, damp_row]
        damp = jnp.concatenate(damp_rows * copies, axis=0)

        def analyse(group, carry):
            for step in range(WAVE_UNROLL):
                wave = group * WAVE_UNROLL + step
                at = pl.ds(pl.multiple_of(wave * rows, rows), rows)
                product = dot(work[at, :].astype(jnp.bfloat16), analysis[wave], 1, 0)
                product = product[:, 0:waves] + product[:, waves:]
                spectral = product + pltpu.roll(product, half, 0)
                total[at, :] = total[at, :] + spectral
                if time > 0:
                    damped = spectral * damp
                    part = damped.astype(jnp.bfloat16).astype(jnp.float32)
                    filtered[at, :] = jnp.where(is_high, part, damped - part)
            return carry

        def synthesise(group, carry):
            for step in range(WAVE_UNROLL):
                wave = group * WAVE_UNROLL + step
                at = pl.ds(pl.multiple_of(wave * rows, rows), rows)
                result = dot(filtered[at, :].astype(jnp.bfloat16), synthesis[wave], 1, 0)
                result = result[:, 0:lats] + result[:, lats:]
                work[at, :] = result + pltpu.roll(result, half, 0)
            return carry

        lax.fori_loop(0, waves // WAVE_UNROLL, analyse, 0)
        if time > 0:
            lax.fori_loop(0, waves // WAVE_UNROLL, synthesise, 0)
            for k in range(kept):
                parts = [work[pl.ds(2 * k + p, waves, stride=rows), :].T for p in range(2)]
                synth_high, synth_low = split_parts(jnp.concatenate(parts, axis=1))
                gridded = dot(synth_high, fourier_high[...], 1, 0)
                gridded = gridded + dot(synth_high, fourier_low[...], 1, 0)
                gridded = gridded + dot(synth_low, fourier_high[...], 1, 0)
                here = slice(k * lats, (k + 1) * lats)
                forced[here, :] = tangent[time * kept + k] * forced[here, :] + gridded

    scaled = []
    for k in range(kept):
        for p in range(2):
            scaled.append(
                total[pl.ds(2 * k + p, waves, stride=rows), :] * spread[k : k + 1, :]
            )
    for block in range(times):
        cols = slice(block * degree_block, (block + 1) * degree_block)
        out[block] = jnp.concatenate([piece[:, cols] for piece in scaled], axis=1)


def sweep(forcing, tangent, spread, tables, times):
    kept = spread.shape[0]
    lats, lons = tangent.shape[1:]
    waves = tables[0].shape[0]
    rows = max(SUBLANES, 4 * kept)
    high, low = fourier_rows(lons, waves)
    return pl.pallas_call(
        sweep_kernel,
        out_shape=jax.ShapeDtypeStruct((times, waves, 2 * kept * waves // times), jnp.float32),
        in_specs=[vmem()] * 7,
        out_specs=vmem(),
        scratch_shapes=[
            pltpu.VMEM((kept * lats, lons), jnp.float32),
            pltpu.VMEM((waves * rows, lats), jnp.float32),
            pltpu.VMEM((waves * rows, waves), jnp.float32),
            pltpu.VMEM((waves * rows, waves), jnp.float32),
        ],
        compiler_params=pltpu.CompilerParams(vmem_limit_bytes=50 * 2**20),
        name="sweep",
    )(forcing, tangent, spread, high, low, *tables)


def shards(obs_cell, innovation, tangent, damping, spread, vertical):
    sections = lax.axis_size("tm")
    groups = lax.axis_size("lev")
    my_section = lax.axis_index("tm")
    my_group = lax.axis_index("lev")
    lev_dev, lat_rows, lon_cols = tangent.shape[1:]
    wave_count = damping.shape[2]
    repeat = max(1, sections // lev_dev)
    kept = max(1, lev_dev // sections)
    my_first = my_group * lev_dev + (my_section // repeat) * kept

    def exchange(field):
        field = jnp.repeat(field, repeat, axis=0) if repeat > 1 else field
        return lax.all_to_all(field, "tm", split_axis=0, concat_axis=0, tiled=True)

    tangent_mine = exchange(tangent[0])
    damp_here = lax.dynamic_slice_in_dim(damping[0], my_group * lev_dev, lev_dev, 0)
    forcing = forcing_field(obs_cell[0], innovation[0], damp_here, lat_rows, lon_cols)
    forcing_mine = exchange(forcing)
    tables = legendre_tables(lat_rows, wave_count)
    spread_mine = lax.dynamic_slice_in_dim(spread, my_first, kept, 0)
    blocks = sweep(forcing_mine, tangent_mine, spread_mine, tables, sections)

    block_waves = wave_count // groups
    block_degrees = wave_count // sections
    blocks = blocks.reshape(sections * groups, block_waves, 2 * kept * block_degrees)
    owned = lax.all_to_all(blocks, ("tm", "lev"), split_axis=0, concat_axis=0, tiled=True)
    owned = owned.reshape(sections, groups, block_waves, kept, 2, block_degrees)[::repeat]
    mixing = vertical.reshape(groups, sections // repeat, kept, vertical.shape[1])
    return jnp.einsum("gukl,ugmkpn->lmpn", mixing, owned, precision=PRECISE)


def solution(mesh):
    placed = (
        P("tm", None),
        P("tm", "lev", None),
        P("tm", "lev", None, None),
        P("tm", None, None),
        P(),
        P(),
    )
    return jax.shard_map(
        shards, mesh=mesh, in_specs=placed, out_specs=P(None, "lev", None, "tm"), check_vma=False
    )
```

```python
import functools
import math

import numpy as np

import jax
import jax.numpy as jnp
from jax import lax
from jax.experimental import pallas as pl
from jax.experimental.pallas import tpu as pltpu
from jax.sharding import PartitionSpec as P


PRECISE = lax.Precision.HIGHEST
LANES = 128
SUBLANES = 8
ACCUMULATORS = 8
OBS_BLOCK = 512
WAVE_UNROLL = 16
DEGREE_UNROLL = 16
SWEEP_MIB = 20


def vmem():
    return pl.BlockSpec(memory_space=pltpu.VMEM)


def smem():
    return pl.BlockSpec(memory_space=pltpu.SMEM)


def in_hbm(*arrays):
    return [pltpu.with_memory_space_constraint(array, pltpu.HBM) for array in arrays]


def fourier_rows(lon_count, wave_count):
    longitude = np.arange(lon_count)[None, :]
    wavenumber = np.arange(wave_count)[:, None]
    angles = (longitude * wavenumber % lon_count) * (2.0 * math.pi / lon_count)
    rows = np.concatenate([np.cos(angles), np.sin(angles)]) * math.sqrt(2.0 / lon_count)
    rows = rows.astype(np.float32)
    high = rows.astype(jnp.bfloat16)
    low = (rows - high.astype(np.float32)).astype(jnp.bfloat16)
    return high, low


def legendre_seeds(lat_count, wave_count):
    orders = np.arange(wave_count, dtype=np.float64)[:, None]
    degrees = np.arange(wave_count, dtype=np.float64)[None, :]
    latitude = (np.arange(lat_count) + 0.5) * (math.pi / lat_count) - 0.5 * math.pi
    sine = np.sin(latitude)[None, :]
    cosine = np.cos(latitude)[None, :]
    gammas = np.array(
        [
            math.lgamma(order + 1.5) - math.lgamma(1.5) - math.lgamma(order + 1.0)
            for order in range(wave_count)
        ]
    )[:, None]
    diagonal = np.exp(-0.5 * math.log(2.0) + 0.5 * gammas + orders * np.log(cosine))
    diagonal = diagonal * np.sqrt(math.pi / lat_count * cosine)
    upward = np.sqrt(
        np.maximum(4.0 * degrees**2 - 1.0, 1.0) / np.maximum(degrees**2 - orders**2, 1.0)
    )
    lower = degrees - 1.0
    downward = np.sqrt(
        np.maximum(lower**2 - orders**2, 0.0) / np.maximum(4.0 * lower**2 - 1.0, 1.0)
    )
    sine = np.broadcast_to(sine, (SUBLANES, lat_count))
    return np.concatenate([upward, upward * downward, diagonal, sine]).astype(np.float32)


def split_parts(values):
    high = values.astype(jnp.bfloat16)
    low = (values - high.astype(jnp.float32)).astype(jnp.bfloat16)
    return high, low


def dot(left, right, left_dim, right_dim):
    return lax.dot_general(
        left, right, (((left_dim,), (right_dim,)), ((), ())), preferred_element_type=jnp.float32
    )


def legendre_kernel(seeds, analysis, synthesis, up_now, down_now, values):
    waves, lats = analysis.shape[:2]
    pitch = values.shape[0] // waves
    up_now[...] = seeds[0:waves, :]
    down_now[...] = seeds[waves : 2 * waves, :]
    order = lax.broadcasted_iota(jnp.int32, (waves, lats), 0)
    sine_rows = jnp.broadcast_to(seeds[3 * waves : 3 * waves + 1, :], (waves, lats))

    def advance(group, state):
        one, two = state
        up = up_now[...]
        down = down_now[...]
        for step in range(DEGREE_UNROLL):
            degree = group * DEGREE_UNROLL + step
            seed = jnp.where(order == degree, seeds[2 * waves : 3 * waves, :], 0.0)
            current = (up[:, step : step + 1] * sine_rows) * one
            current = current - down[:, step : step + 1] * two + seed
            values[pl.ds(pl.multiple_of(degree * pitch, SUBLANES), waves), :] = current
            one, two = current, one
        up_now[...] = pltpu.roll(up, waves - DEGREE_UNROLL, 1)
        down_now[...] = pltpu.roll(down, waves - DEGREE_UNROLL, 1)
        return one, two

    zeros = jnp.zeros((waves, lats), jnp.float32)
    lax.fori_loop(0, waves // DEGREE_UNROLL, advance, (zeros, zeros))

    def emit(wave, carry):
        rows = values[pl.ds(wave, waves, stride=pitch), :]
        analysis[wave] = jnp.concatenate(split_parts(rows.T), axis=1)
        synthesis[wave] = jnp.concatenate(split_parts(rows), axis=1)
        return carry

    lax.fori_loop(0, waves, emit, 0, unroll=4)


def legendre_tables(lat_count, wave_count):
    pitch = wave_count + SUBLANES
    return pl.pallas_call(
        legendre_kernel,
        out_shape=[
            jax.ShapeDtypeStruct((wave_count, lat_count, 2 * wave_count), jnp.bfloat16),
            jax.ShapeDtypeStruct((wave_count, wave_count, 2 * lat_count), jnp.bfloat16),
        ],
        in_specs=[vmem()],
        out_specs=[vmem()] * 2,
        scratch_shapes=[
            pltpu.VMEM((wave_count, wave_count), jnp.float32),
            pltpu.VMEM((wave_count, wave_count), jnp.float32),
            pltpu.VMEM((wave_count * pitch, lat_count), jnp.float32),
        ],
        compiler_params=pltpu.CompilerParams(vmem_limit_bytes=12 * 2**20),
        name="legendre",
    )(*in_hbm(legendre_seeds(lat_count, wave_count)))


def scatter_kernel(rows, cells, innov, damping, *refs, sections):
    levels, obs = innov.shape
    waves = damping.shape[1]
    outs = refs[:sections]
    field, even, odd, sems = refs[sections : sections + 4]
    sums = refs[sections + 4 :]
    lats = field.shape[1] - SUBLANES
    lons = field.shape[2]
    span = LANES // levels
    for part in sums:
        part[...] = jnp.zeros(part.shape, jnp.float32)
    row = lax.broadcasted_iota(jnp.int32, (4 * SUBLANES, 2 * LANES), 0)
    lane = lax.broadcasted_iota(jnp.int32, (4 * SUBLANES, 2 * LANES), 1)
    values_here = (row < 3 * SUBLANES) & (lane < LANES) & (row % SUBLANES == lane // span)
    place = (values_here | ((row == 3 * SUBLANES) & (lane >= LANES))).astype(jnp.bfloat16)
    lane_low = (lax.broadcasted_iota(jnp.int32, (OBS_BLOCK, LANES), 1) % span).astype(jnp.float32)

    def spread_out(block, data):
        start = pl.multiple_of(block * OBS_BLOCK, OBS_BLOCK)
        rest = innov[:, pl.ds(start, OBS_BLOCK)]
        if levels < SUBLANES:
            fill = jnp.zeros((SUBLANES - levels, OBS_BLOCK), jnp.float32)
            rest = jnp.concatenate([rest, fill], axis=0)
        parts = []
        for _ in range(3):
            parts.append(rest.astype(jnp.bfloat16).astype(jnp.float32))
            rest = rest - parts[-1]
        low = (cells[:, pl.ds(start, OBS_BLOCK)] // lons % span).astype(jnp.float32)
        parts.append(jnp.broadcast_to(low, (SUBLANES, OBS_BLOCK)))
        stacked = jnp.concatenate(parts, axis=0).astype(jnp.bfloat16)
        placed = dot(stacked, place, 0, 0)
        data[...] = jnp.where(placed[:, LANES:] == lane_low, placed[:, :LANES], 0.0)

    def add_rows(block, data):
        start = pl.multiple_of(block * OBS_BLOCK, OBS_BLOCK)
        for step in range(OBS_BLOCK):
            part = sums[step % ACCUMULATORS]
            at = pl.ds(rows[start + step], 1)
            part[at, :] = part[at, :] + data[step : step + 1, :]

    blocks = obs // OBS_BLOCK
    spread_out(0, even)

    def two_blocks(pair, carry):
        spread_out(2 * pair + 1, odd)
        add_rows(2 * pair, even)
        spread_out(jnp.minimum(2 * pair + 2, blocks - 1), even)
        add_rows(2 * pair + 1, odd)
        return carry

    lax.fori_loop(0, blocks // 2, two_blocks, 0)

    for high in range(lats // span):
        for west in range(lons // LANES):
            block = pl.ds(high * lons + west * LANES, LANES)
            total = sums[0][block, :]
            for part in sums[1:]:
                total = total + part[block, :]
            turned = total.T
            for k in range(levels):
                field[k, high * span : (high + 1) * span, west * LANES : (west + 1) * LANES] = (
                    turned[k * span : (k + 1) * span, :]
                )
    field[:, lats:, :] = jnp.zeros((levels, SUBLANES, lons), jnp.float32)
    first = lax.axis_index("lev") * levels
    for k in range(levels):
        field[k, lats : lats + 1, 0:waves] = damping[pl.ds(first + k, 1), :]
    me = lax.axis_index("tm")
    chunk = max(1, levels // sections)
    repeat = max(1, sections // levels)
    copies = [
        pltpu.make_async_copy(
            field.at[pl.ds(((me ^ slot) // repeat) * chunk, chunk)], outs[slot], sems.at[slot]
        )
        for slot in range(sections)
    ]
    for copy in copies:
        copy.start()
    for copy in copies:
        copy.wait()


def cut_kernel(field, *refs, sections):
    outs, sems = refs[:sections], refs[sections]
    levels = field.shape[0]
    me = lax.axis_index("tm")
    chunk = max(1, levels // sections)
    repeat = max(1, sections // levels)
    copies = [
        pltpu.make_async_copy(
            field.at[pl.ds(((me ^ slot) // repeat) * chunk, chunk)], outs[slot], sems.at[slot]
        )
        for slot in range(sections)
    ]
    for copy in copies:
        copy.start()
    for copy in copies:
        copy.wait()


def cut_chunks(field, sections):
    levels, lats, lons = field.shape
    chunk = max(1, levels // sections)
    return pl.pallas_call(
        functools.partial(cut_kernel, sections=sections),
        out_shape=[jax.ShapeDtypeStruct((chunk, lats, lons), jnp.float32)] * sections,
        in_specs=[pl.BlockSpec(memory_space=pl.ANY)],
        out_specs=[vmem()] * sections,
        scratch_shapes=[pltpu.SemaphoreType.DMA((sections,))],
        compiler_params=pltpu.CompilerParams(vmem_limit_bytes=4 * 2**20),
        name="cut",
    )(field)


def forcing_chunks(cells, innov, damping, lats, lons, sections):
    levels, _ = innov.shape
    span = LANES // levels
    rows = (cells // (lons * span)) * lons + cells % lons
    chunk = max(1, levels // sections)
    return pl.pallas_call(
        functools.partial(scatter_kernel, sections=sections),
        out_shape=[jax.ShapeDtypeStruct((chunk, lats + SUBLANES, lons), jnp.float32)] * sections,
        in_specs=[smem(), vmem(), vmem(), vmem()],
        out_specs=[pl.BlockSpec(memory_space=pl.ANY)] * sections,
        scratch_shapes=[
            pltpu.VMEM((levels, lats + SUBLANES, lons), jnp.float32),
            pltpu.VMEM((OBS_BLOCK, LANES), jnp.float32),
            pltpu.VMEM((OBS_BLOCK, LANES), jnp.float32),
            pltpu.SemaphoreType.DMA((sections,)),
        ]
        + [pltpu.VMEM((lats * lons // span, LANES), jnp.float32)] * ACCUMULATORS,
        compiler_params=pltpu.CompilerParams(vmem_limit_bytes=32 * 2**20),
        name="scatter",
    )(rows, *in_hbm(cells[None, :], innov, damping))


def sweep_kernel(spread, fourier, analysis, synthesis, *refs, sections):
    chunks, tangents = refs[:sections], refs[sections : 2 * sections]
    out, forced, work, filtered, total, damp_now = refs[2 * sections :]
    fourier_high, fourier_low = fourier.at[0], fourier.at[1]
    waves, lats = analysis.shape[:2]
    times = sections
    degree_block = waves // times
    kept = chunks[0].shape[0]
    levels = spread.shape[0] // lax.axis_size("lev")
    half = 2 * kept
    rows = max(SUBLANES, 2 * half)
    copies = rows // half
    row = lax.broadcasted_iota(jnp.int32, (rows, waves), 0)
    is_high = (row // half) % 2 == 0
    total[...] = jnp.zeros(total.shape, jnp.float32)
    forced[...] = jnp.zeros(forced.shape, jnp.float32)
    me = lax.axis_index("tm")

    for time in range(times - 1, -1, -1):
        for slot in range(sections):

            @pl.when(me ^ slot == time)
            def _(chunk=chunks[slot]):
                for k in range(kept):
                    here = slice(k * lats, (k + 1) * lats)
                    forced[here, :] = forced[here, :] + chunk[k, 0:lats, :]
                    damp_now[k : k + 1, :] = chunk[k, lats : lats + 1, 0:waves]

        high, low = split_parts(forced[...])
        coeffs = dot(fourier_high[...], high, 1, 1)
        coeffs = coeffs + dot(fourier_low[...], high, 1, 1)
        coeffs = coeffs + dot(fourier_high[...], low, 1, 1)
        for k in range(kept):
            for p in range(2):
                piece = coeffs[p * waves : (p + 1) * waves, k * lats : (k + 1) * lats]
                piece_high = piece.astype(jnp.bfloat16).astype(jnp.float32)
                piece_low = piece - piece_high
                for copy in range(copies):
                    at = copy * half + 2 * k + p
                    work[pl.ds(at, waves, stride=rows), :] = (
                        piece_high if copy % 2 == 0 else piece_low
                    )
        damp_rows = []
        for k in range(kept):
            damp_row = damp_now[k : k + 1, :]
            damp_rows += [damp_row, damp_row]
        damp = jnp.concatenate(damp_rows * copies, axis=0)

        def analyse(group, carry):
            for step in range(WAVE_UNROLL):
                wave = group * WAVE_UNROLL + step
                at = pl.ds(pl.multiple_of(wave * rows, rows), rows)
                product = dot(work[at, :].astype(jnp.bfloat16), analysis[wave], 1, 0)
                product = product[:, 0:waves] + product[:, waves:]
                spectral = product + pltpu.roll(product, half, 0)
                total[at, :] = total[at, :] + spectral
                if time > 0:
                    damped = spectral * damp
                    part = damped.astype(jnp.bfloat16).astype(jnp.float32)
                    filtered[at, :] = jnp.where(is_high, part, damped - part)
            return carry

        def synthesise(group, carry):
            for step in range(WAVE_UNROLL):
                wave = group * WAVE_UNROLL + step
                at = pl.ds(pl.multiple_of(wave * rows, rows), rows)
                result = dot(filtered[at, :].astype(jnp.bfloat16), synthesis[wave], 1, 0)
                result = result[:, 0:lats] + result[:, lats:]
                work[at, :] = result + pltpu.roll(result, half, 0)
            return carry

        lax.fori_loop(0, waves // WAVE_UNROLL, analyse, 0)
        if time > 0:
            for slot in range(sections):

                @pl.when(me ^ slot == time)
                def _(factor=tangents[slot]):
                    for k in range(kept):
                        here = slice(k * lats, (k + 1) * lats)
                        forced[here, :] = factor[k] * forced[here, :]

            lax.fori_loop(0, waves // WAVE_UNROLL, synthesise, 0)
            for k in range(kept):
                parts = [work[pl.ds(2 * k + p, waves, stride=rows), :].T for p in range(2)]
                synth_high, synth_low = split_parts(jnp.concatenate(parts, axis=1))
                gridded = dot(synth_high, fourier_high[...], 1, 0)
                gridded = gridded + dot(synth_high, fourier_low[...], 1, 0)
                gridded = gridded + dot(synth_low, fourier_high[...], 1, 0)
                here = slice(k * lats, (k + 1) * lats)
                forced[here, :] = forced[here, :] + gridded

    scaled = []
    repeat = max(1, sections // levels)
    first = lax.axis_index("lev") * levels + (me // repeat) * kept
    for k in range(kept):
        factor = spread[pl.ds(first + k, 1), :]
        for p in range(2):
            scaled.append(total[pl.ds(2 * k + p, waves, stride=rows), :] * factor)
    for block in range(times):
        cols = slice(block * degree_block, (block + 1) * degree_block)
        out[block] = jnp.concatenate([piece[:, cols] for piece in scaled], axis=1)


def sweep(chunks, tangents, spread, tables):
    sections = len(chunks)
    kept = chunks[0].shape[0]
    lats, lons = tangents[0].shape[1:]
    waves = tables[0].shape[0]
    rows = max(SUBLANES, 4 * kept)
    fourier = np.stack(fourier_rows(lons, waves))
    return pl.pallas_call(
        functools.partial(sweep_kernel, sections=sections),
        out_shape=jax.ShapeDtypeStruct(
            (sections, waves, 2 * kept * waves // sections), jnp.float32
        ),
        in_specs=[vmem()] * (4 + 2 * sections),
        out_specs=vmem(),
        scratch_shapes=[
            pltpu.VMEM((kept * lats, lons), jnp.float32),
            pltpu.VMEM((waves * rows, lats), jnp.float32),
            pltpu.VMEM((waves * rows, waves), jnp.float32),
            pltpu.VMEM((waves * rows, waves), jnp.float32),
            pltpu.VMEM((SUBLANES, waves), jnp.float32),
        ],
        compiler_params=pltpu.CompilerParams(vmem_limit_bytes=SWEEP_MIB * 2**20),
        name="sweep",
    )(*in_hbm(spread, fourier), *tables, *chunks, *tangents)


def shards(obs_cell, innovation, tangent, damping, spread, vertical):
    sections = lax.axis_size("tm")
    groups = lax.axis_size("lev")
    lev_dev, lat_rows, lon_cols = tangent.shape[1:]
    wave_count = damping.shape[2]
    repeat = max(1, sections // lev_dev)
    kept = max(1, lev_dev // sections)

    def exchange(chunks):
        return [
            lax.ppermute(chunk, "tm", [(i, i ^ slot) for i in range(sections)]) if slot else chunk
            for slot, chunk in enumerate(chunks)
        ]

    cut = cut_chunks(*in_hbm(tangent[0]), sections)
    tangents = exchange(cut)
    chunks = forcing_chunks(obs_cell[0], innovation[0], damping[0], lat_rows, lon_cols, sections)
    chunks = exchange(chunks)
    tables = legendre_tables(lat_rows, wave_count)
    blocks = sweep(chunks, tangents, spread, tables)

    block_waves = wave_count // groups
    block_degrees = wave_count // sections
    blocks = blocks.reshape(sections * groups, block_waves, 2 * kept * block_degrees)
    owned = lax.all_to_all(blocks, ("tm", "lev"), split_axis=0, concat_axis=0, tiled=True)
    owned = owned.reshape(sections, groups, block_waves, kept, 2, block_degrees)[::repeat]
    mixing = vertical.reshape(groups, sections // repeat, kept, vertical.shape[1])
    return jnp.einsum("gukl,ugmkpn->lmpn", mixing, owned, precision=PRECISE)


def solution(mesh):
    placed = (
        P("tm", None),
        P("tm", "lev", None),
        P("tm", "lev", None, None),
        P("tm", None, None),
        P(),
        P(),
    )
    return jax.shard_map(
        shards, mesh=mesh, in_specs=placed, out_specs=P(None, "lev", None, "tm"), check_vma=False
    )
```

```python
import functools
import math

import numpy as np

import jax
import jax.numpy as jnp
from jax import lax
from jax.experimental import pallas as pl
from jax.experimental.pallas import tpu as pltpu
from jax.sharding import PartitionSpec as P


LANES = 128
SUBLANES = 8
ACCUMULATORS = 8
OBS_BLOCK = 512
WAVE_UNROLL = 16
DEGREE_BLOCK = 16
SWEEP_MIB = 20


def vmem():
    return pl.BlockSpec(memory_space=pltpu.VMEM)


def smem():
    return pl.BlockSpec(memory_space=pltpu.SMEM)


def in_hbm(*arrays):
    return [pltpu.with_memory_space_constraint(array, pltpu.HBM) for array in arrays]


def fourier_rows(lon_count, wave_count):
    longitude = np.arange(lon_count)[None, :]
    wavenumber = np.arange(wave_count)[:, None]
    angles = (longitude * wavenumber % lon_count) * (2.0 * math.pi / lon_count)
    rows = np.concatenate([np.cos(angles), np.sin(angles)]) * math.sqrt(2.0 / lon_count)
    rows = rows.astype(np.float32)
    high = rows.astype(jnp.bfloat16)
    low = (rows - high.astype(np.float32)).astype(jnp.bfloat16)
    return high, low


def legendre_seeds(lat_count, wave_count):
    orders = np.arange(wave_count, dtype=np.float64)[:, None]
    degrees = np.arange(wave_count, dtype=np.float64)[None, :]
    latitude = (np.arange(lat_count) + 0.5) * (math.pi / lat_count) - 0.5 * math.pi
    sine = np.sin(latitude)[None, :]
    cosine = np.cos(latitude)[None, :]
    gammas = np.array(
        [
            math.lgamma(order + 1.5) - math.lgamma(1.5) - math.lgamma(order + 1.0)
            for order in range(wave_count)
        ]
    )[:, None]
    diagonal = np.exp(-0.5 * math.log(2.0) + 0.5 * gammas + orders * np.log(cosine))
    diagonal = diagonal * np.sqrt(math.pi / lat_count * cosine)
    upward = np.sqrt(
        np.maximum(4.0 * degrees**2 - 1.0, 1.0) / np.maximum(degrees**2 - orders**2, 1.0)
    )
    lower = degrees - 1.0
    downward = np.sqrt(
        np.maximum(lower**2 - orders**2, 0.0) / np.maximum(4.0 * lower**2 - 1.0, 1.0)
    )
    sine = np.broadcast_to(sine, (SUBLANES, lat_count))
    return np.concatenate([upward, upward * downward, diagonal, sine]).astype(np.float32)


def split_parts(values):
    high = values.astype(jnp.bfloat16)
    low = (values - high.astype(jnp.float32)).astype(jnp.bfloat16)
    return high, low


def dot(left, right, left_dim, right_dim):
    return lax.dot_general(
        left, right, (((left_dim,), (right_dim,)), ((), ())), preferred_element_type=jnp.float32
    )


def legendre_kernel(
    seeds, fourier, spread, analysis, synthesis, fourier_near, spread_near, values, sems
):
    waves, lats = analysis.shape[:2]
    pitch = values.shape[0] // waves
    nearer = [
        pltpu.make_async_copy(fourier, fourier_near, sems.at[0]),
        pltpu.make_async_copy(spread, spread_near, sems.at[1]),
    ]
    for copy in nearer:
        copy.start()
    sine = seeds[3 * waves : 3 * waves + 1, :]
    one = jnp.zeros((0, lats), jnp.float32)
    two = one
    for degree in range(waves):
        live = (degree // DEGREE_BLOCK + 1) * DEGREE_BLOCK
        if one.shape[0] < live:
            fresh = jnp.zeros((live - one.shape[0], lats), jnp.float32)
            one = jnp.concatenate([one, fresh], axis=0) if one.shape[0] else fresh
            two = jnp.concatenate([two, fresh], axis=0) if two.shape[0] else fresh
        order = lax.broadcasted_iota(jnp.int32, (DEGREE_BLOCK, lats), 0) + (live - DEGREE_BLOCK)
        edge = slice(2 * waves + live - DEGREE_BLOCK, 2 * waves + live)
        seed = jnp.where(order == degree, seeds[edge, :], 0.0)
        if live > DEGREE_BLOCK:
            seed = jnp.concatenate(
                [jnp.zeros((live - DEGREE_BLOCK, lats), jnp.float32), seed], axis=0
            )
        up = seeds[0:live, degree : degree + 1]
        down = seeds[waves : waves + live, degree : degree + 1]
        current = (up * sine) * one - down * two + seed
        values[degree * pitch : degree * pitch + live, :] = current
        one, two = current, one

    row = lax.broadcasted_iota(jnp.int32, (lats, lats), 0)
    identity = (row == lax.broadcasted_iota(jnp.int32, (lats, lats), 1)).astype(jnp.bfloat16)
    for group in range(waves // DEGREE_BLOCK):
        skipped = group * DEGREE_BLOCK

        def emit(quad, carry):
            for step in range(4):
                wave = skipped + 4 * quad + step
                start = skipped * pitch + wave
                rows = values[pl.ds(start, waves - skipped, stride=pitch), :]
                if skipped:
                    rows = jnp.concatenate(
                        [jnp.zeros((skipped, lats), jnp.float32), rows], axis=0
                    )
                high, low = split_parts(rows)
                synthesis[wave] = jnp.concatenate([high, low], axis=1)
                if step % 2:
                    both = jnp.concatenate([high, low], axis=0)
                    analysis[wave] = dot(identity, both, 1, 1).astype(jnp.bfloat16)
                else:
                    analysis[wave] = jnp.concatenate(split_parts(rows.T), axis=1)
            return carry

        lax.fori_loop(0, DEGREE_BLOCK // 4, emit, 0)
    for copy in nearer:
        copy.wait()


def legendre_tables(lat_count, lon_count, wave_count, spread):
    pitch = wave_count + SUBLANES
    fourier = np.stack(fourier_rows(lon_count, wave_count))
    anywhere = pl.BlockSpec(memory_space=pl.ANY)
    return pl.pallas_call(
        legendre_kernel,
        out_shape=[
            jax.ShapeDtypeStruct((wave_count, lat_count, 2 * wave_count), jnp.bfloat16),
            jax.ShapeDtypeStruct((wave_count, wave_count, 2 * lat_count), jnp.bfloat16),
            jax.ShapeDtypeStruct(fourier.shape, jnp.bfloat16),
            jax.ShapeDtypeStruct(spread.shape, jnp.float32),
        ],
        in_specs=[vmem(), anywhere, anywhere],
        out_specs=[vmem()] * 4,
        scratch_shapes=[
            pltpu.VMEM((wave_count * pitch, lat_count), jnp.float32),
            pltpu.SemaphoreType.DMA((2,)),
        ],
        compiler_params=pltpu.CompilerParams(vmem_limit_bytes=14 * 2**20),
        name="legendre",
    )(*in_hbm(legendre_seeds(lat_count, wave_count), fourier, spread))


def scatter_kernel(rows, cells, innov, damping, *refs, sections, lats, lons):
    levels, obs = innov.shape
    outs = refs[:sections]
    field, even, odd, sems = refs[sections : sections + 4]
    sums = refs[sections + 4 :]
    span = LANES // levels
    chunk = max(1, levels // sections)
    for part in sums:
        part[...] = jnp.zeros(part.shape, jnp.float32)
    row = lax.broadcasted_iota(jnp.int32, (4 * SUBLANES, 2 * LANES), 0)
    lane = lax.broadcasted_iota(jnp.int32, (4 * SUBLANES, 2 * LANES), 1)
    values_here = (row < 3 * SUBLANES) & (lane < LANES) & (row % SUBLANES == lane // span)
    place = (values_here | ((row == 3 * SUBLANES) & (lane >= LANES))).astype(jnp.bfloat16)
    lane_low = (lax.broadcasted_iota(jnp.int32, (OBS_BLOCK, LANES), 1) % span).astype(jnp.float32)

    def spread_out(block, data):
        start = pl.multiple_of(block * OBS_BLOCK, OBS_BLOCK)
        rest = innov[:, pl.ds(start, OBS_BLOCK)]
        if levels < SUBLANES:
            fill = jnp.zeros((SUBLANES - levels, OBS_BLOCK), jnp.float32)
            rest = jnp.concatenate([rest, fill], axis=0)
        parts = []
        for _ in range(3):
            parts.append(rest.astype(jnp.bfloat16).astype(jnp.float32))
            rest = rest - parts[-1]
        low = (cells[:, pl.ds(start, OBS_BLOCK)] // lons % span).astype(jnp.float32)
        parts.append(jnp.broadcast_to(low, (SUBLANES, OBS_BLOCK)))
        stacked = jnp.concatenate(parts, axis=0).astype(jnp.bfloat16)
        placed = dot(stacked, place, 0, 0)
        data[...] = jnp.where(placed[:, LANES:] == lane_low, placed[:, :LANES], 0.0)

    def add_rows(block, data):
        start = pl.multiple_of(block * OBS_BLOCK, OBS_BLOCK)
        for step in range(OBS_BLOCK):
            part = sums[step % ACCUMULATORS]
            at = pl.ds(rows[start + step], 1)
            part[at, :] = part[at, :] + data[step : step + 1, :]

    blocks = obs // OBS_BLOCK
    spread_out(0, even)

    def two_blocks(pair, carry):
        spread_out(2 * pair + 1, odd)
        add_rows(2 * pair, even)
        spread_out(jnp.minimum(2 * pair + 2, blocks - 1), even)
        add_rows(2 * pair + 1, odd)
        return carry

    lax.fori_loop(0, blocks // 2, two_blocks, 0)

    first = lax.axis_index("lev") * levels
    for high in range(lats // span):
        for west in range(lons // LANES):
            block = pl.ds(high * lons + west * LANES, LANES)
            total = sums[0][block, :]
            for part in sums[1:]:
                total = total + part[block, :]
            turned = total.T
            for k in range(levels):
                at = ((k % chunk) * (lons // LANES) + west) * lats + high * span
                field[k // chunk, at : at + span, :] = turned[k * span : (k + 1) * span, :]
    tail = chunk * lats * lons // LANES
    for piece in range(levels // chunk):
        field[piece, tail:, :] = jnp.zeros((SUBLANES, LANES), jnp.float32)
        for k in range(chunk):
            rates = damping[pl.ds(first + piece * chunk + k, 1), :]
            field[piece, tail + k : tail + k + 1, :] = rates
    me = lax.axis_index("tm")
    repeat = max(1, sections // levels)
    copies = [
        pltpu.make_async_copy(field.at[(me ^ slot) // repeat], outs[slot], sems.at[slot])
        for slot in range(sections)
    ]
    for copy in copies:
        copy.start()
    for copy in copies:
        copy.wait()


def cut_kernel(field, *refs, sections):
    outs, sems = refs[:sections], refs[sections]
    levels = field.shape[0]
    me = lax.axis_index("tm")
    chunk = max(1, levels // sections)
    repeat = max(1, sections // levels)
    copies = [
        pltpu.make_async_copy(
            field.at[pl.ds(((me ^ slot) // repeat) * chunk, chunk)], outs[slot], sems.at[slot]
        )
        for slot in range(sections)
    ]
    for copy in copies:
        copy.start()
    for copy in copies:
        copy.wait()


def cut_chunks(field, sections):
    levels, lats, lons = field.shape
    chunk = max(1, levels // sections)
    return pl.pallas_call(
        functools.partial(cut_kernel, sections=sections),
        out_shape=[jax.ShapeDtypeStruct((chunk, lats, lons), jnp.float32)] * sections,
        in_specs=[pl.BlockSpec(memory_space=pl.ANY)],
        out_specs=[vmem()] * sections,
        scratch_shapes=[pltpu.SemaphoreType.DMA((sections,))],
        compiler_params=pltpu.CompilerParams(vmem_limit_bytes=4 * 2**20),
        name="cut",
    )(field)


def forcing_chunks(cells, innov, damping, lats, lons, sections):
    levels, _ = innov.shape
    span = LANES // levels
    rows = (cells // (lons * span)) * lons + cells % lons
    chunk = max(1, levels // sections)
    size = chunk * lats * lons // LANES + SUBLANES
    return pl.pallas_call(
        functools.partial(scatter_kernel, sections=sections, lats=lats, lons=lons),
        out_shape=[jax.ShapeDtypeStruct((size, LANES), jnp.float32)] * sections,
        in_specs=[smem(), vmem(), vmem(), vmem()],
        out_specs=[pl.BlockSpec(memory_space=pl.ANY)] * sections,
        scratch_shapes=[
            pltpu.VMEM((levels // chunk, size, LANES), jnp.float32),
            pltpu.VMEM((OBS_BLOCK, LANES), jnp.float32),
            pltpu.VMEM((OBS_BLOCK, LANES), jnp.float32),
            pltpu.SemaphoreType.DMA((sections,)),
        ]
        + [pltpu.VMEM((lats * lons // span, LANES), jnp.float32)] * ACCUMULATORS,
        compiler_params=pltpu.CompilerParams(vmem_limit_bytes=32 * 2**20),
        name="scatter",
    )(rows, *in_hbm(cells[None, :], innov, damping))


def sweep_kernel(analysis, synthesis, fourier, spread, *refs, sections):
    chunks, tangents = refs[:sections], refs[sections : 2 * sections]
    out, forced, work, filtered, total, damp_now = refs[2 * sections :]
    fourier_high, fourier_low = fourier.at[0], fourier.at[1]
    waves, lats = analysis.shape[:2]
    times = sections
    degree_block = waves // times
    kept = tangents[0].shape[0]
    lons = tangents[0].shape[2]
    levels = spread.shape[0] // lax.axis_size("lev")
    half = 2 * kept
    rows = max(SUBLANES, 2 * half)
    copies = rows // half
    row = lax.broadcasted_iota(jnp.int32, (rows, waves), 0)
    is_high = (row // half) % 2 == 0
    total[...] = jnp.zeros(total.shape, jnp.float32)
    forced[...] = jnp.zeros(forced.shape, jnp.float32)
    me = lax.axis_index("tm")

    for time in range(times - 1, -1, -1):
        for slot in range(sections):

            @pl.when(me ^ slot == time)
            def _(chunk=chunks[slot]):
                for k in range(kept):
                    here = slice(k * lats, (k + 1) * lats)
                    for west in range(lons // LANES):
                        there = slice(west * LANES, (west + 1) * LANES)
                        at = (k * (lons // LANES) + west) * lats
                        forced[here, there] = forced[here, there] + chunk[at : at + lats, :]
                    tail = kept * lats * lons // LANES + k
                    damp_now[k : k + 1, :] = chunk[tail : tail + 1, :]

        high, low = split_parts(forced[...])
        coeffs = dot(fourier_high[...], high, 1, 1)
        coeffs = coeffs + dot(fourier_low[...], high, 1, 1)
        coeffs = coeffs + dot(fourier_high[...], low, 1, 1)
        for k in range(kept):
            for p in range(2):
                piece = coeffs[p * waves : (p + 1) * waves, k * lats : (k + 1) * lats]
                piece_high = piece.astype(jnp.bfloat16).astype(jnp.float32)
                piece_low = piece - piece_high
                for copy in range(copies):
                    at = copy * half + 2 * k + p
                    work[pl.ds(at, waves, stride=rows), :] = (
                        piece_high if copy % 2 == 0 else piece_low
                    )
        damp_rows = []
        for k in range(kept):
            damp_row = damp_now[k : k + 1, :]
            damp_rows += [damp_row, damp_row]
        damp = jnp.concatenate(damp_rows * copies, axis=0)

        def analyse(group, carry):
            for step in range(WAVE_UNROLL):
                wave = group * WAVE_UNROLL + step
                at = pl.ds(pl.multiple_of(wave * rows, rows), rows)
                product = dot(work[at, :].astype(jnp.bfloat16), analysis[wave], 1, 0)
                product = product[:, 0:waves] + product[:, waves:]
                spectral = product + pltpu.roll(product, half, 0)
                total[at, :] = total[at, :] + spectral
                if time > 0:
                    damped = spectral * damp
                    part = damped.astype(jnp.bfloat16).astype(jnp.float32)
                    filtered[at, :] = jnp.where(is_high, part, damped - part)
            return carry

        def synthesise(group, carry):
            for step in range(WAVE_UNROLL):
                wave = group * WAVE_UNROLL + step
                at = pl.ds(pl.multiple_of(wave * rows, rows), rows)
                result = dot(filtered[at, :].astype(jnp.bfloat16), synthesis[wave], 1, 0)
                result = result[:, 0:lats] + result[:, lats:]
                work[at, :] = result + pltpu.roll(result, half, 0)
            return carry

        lax.fori_loop(0, waves // WAVE_UNROLL, analyse, 0)
        if time > 0:
            for slot in range(sections):

                @pl.when(me ^ slot == time)
                def _(factor=tangents[slot]):
                    for k in range(kept):
                        here = slice(k * lats, (k + 1) * lats)
                        forced[here, :] = factor[k] * forced[here, :]

            lax.fori_loop(0, waves // WAVE_UNROLL, synthesise, 0)
            for k in range(kept):
                parts = [work[pl.ds(2 * k + p, waves, stride=rows), :].T for p in range(2)]
                synth_high, synth_low = split_parts(jnp.concatenate(parts, axis=1))
                gridded = dot(synth_high, fourier_high[...], 1, 0)
                gridded = gridded + dot(synth_high, fourier_low[...], 1, 0)
                gridded = gridded + dot(synth_low, fourier_high[...], 1, 0)
                here = slice(k * lats, (k + 1) * lats)
                forced[here, :] = forced[here, :] + gridded

    scaled = []
    repeat = max(1, sections // levels)
    first = lax.axis_index("lev") * levels + (me // repeat) * kept
    for k in range(kept):
        factor = spread[pl.ds(first + k, 1), :]
        for p in range(2):
            scaled.append(total[pl.ds(2 * k + p, waves, stride=rows), :] * factor)
    for block in range(times):
        cols = slice(block * degree_block, (block + 1) * degree_block)
        out[block] = jnp.concatenate([piece[:, cols] for piece in scaled], axis=1)


def sweep(chunks, tangents, tables):
    sections = len(chunks)
    kept, lats, lons = tangents[0].shape
    waves = tables[0].shape[0]
    rows = max(SUBLANES, 4 * kept)
    return pl.pallas_call(
        functools.partial(sweep_kernel, sections=sections),
        out_shape=jax.ShapeDtypeStruct(
            (sections, waves, 2 * kept * waves // sections), jnp.float32
        ),
        in_specs=[vmem()] * (4 + 2 * sections),
        out_specs=vmem(),
        scratch_shapes=[
            pltpu.VMEM((kept * lats, lons), jnp.float32),
            pltpu.VMEM((waves * rows, lats), jnp.float32),
            pltpu.VMEM((waves * rows, waves), jnp.float32),
            pltpu.VMEM((waves * rows, waves), jnp.float32),
            pltpu.VMEM((SUBLANES, waves), jnp.float32),
        ],
        compiler_params=pltpu.CompilerParams(vmem_limit_bytes=SWEEP_MIB * 2**20),
        name="sweep",
    )(*tables, *chunks, *tangents)


def mix_kernel(owned, vertical, out, *, sections, groups, repeat):
    peers = sections * groups
    block_waves = owned.shape[0] // peers
    lanes = owned.shape[1]
    steps = sections // repeat
    levels = vertical.shape[0] // groups
    kept = levels // steps
    each = lanes // kept
    columns = []
    for wave in range(block_waves):
        pieces = [
            owned[pl.ds(step * repeat * groups * block_waves + wave, groups, stride=block_waves), :]
            for step in range(steps)
        ]
        columns.append(jnp.concatenate(pieces, axis=0))
    high, low = split_parts(jnp.concatenate(columns, axis=1))
    left = jnp.concatenate([high, low, high], axis=0)
    for k in range(kept):
        pieces = [
            vertical[pl.ds(step * kept + k, groups, stride=levels), :] for step in range(steps)
        ]
        mix_high, mix_low = split_parts(jnp.concatenate(pieces, axis=0))
        product = dot(left, jnp.concatenate([mix_high, mix_high, mix_low], axis=0), 0, 0)
        for wave in range(block_waves):
            start = wave * lanes + k * each
            piece = product[start : start + each, :]
            out[wave] = piece if k == 0 else out[wave] + piece


def mix(owned, vertical, sections, groups, repeat):
    peers, block_waves, lanes = owned.shape
    steps = sections // repeat
    each = lanes // (vertical.shape[0] // groups // steps)
    return pl.pallas_call(
        functools.partial(mix_kernel, sections=sections, groups=groups, repeat=repeat),
        out_shape=jax.ShapeDtypeStruct((block_waves, each, vertical.shape[1]), jnp.float32),
        in_specs=[vmem()] * 2,
        out_specs=vmem(),
        compiler_params=pltpu.CompilerParams(vmem_limit_bytes=16 * 2**20),
        name="mix",
    )(owned.reshape(peers * block_waves, lanes), vertical)


def shards(obs_cell, innovation, tangent, damping, spread, vertical):
    sections = lax.axis_size("tm")
    groups = lax.axis_size("lev")
    lev_dev, lat_rows, lon_cols = tangent.shape[1:]
    wave_count = damping.shape[2]
    repeat = max(1, sections // lev_dev)
    kept = max(1, lev_dev // sections)

    def exchange(chunks):
        return [
            lax.ppermute(chunk, "tm", [(i, i ^ slot) for i in range(sections)]) if slot else chunk
            for slot, chunk in enumerate(chunks)
        ]

    cut = cut_chunks(*in_hbm(tangent[0]), sections)
    tangents = exchange(cut)
    chunks = forcing_chunks(obs_cell[0], innovation[0], damping[0], lat_rows, lon_cols, sections)
    chunks = exchange(chunks)
    tables = legendre_tables(lat_rows, lon_cols, wave_count, spread)
    blocks = sweep(chunks, tangents, tables)

    block_waves = wave_count // groups
    block_degrees = wave_count // sections
    blocks = blocks.reshape(sections * groups, block_waves, 2 * kept * block_degrees)
    owned = lax.all_to_all(blocks, ("tm", "lev"), split_axis=0, concat_axis=0, tiled=True)
    mixed = mix(owned, vertical, sections, groups, repeat)
    mixed = mixed.reshape(block_waves, 2, block_degrees, vertical.shape[1])
    return jnp.transpose(mixed, (3, 0, 1, 2))


def solution(mesh):
    placed = (
        P("tm", None),
        P("tm", "lev", None),
        P("tm", "lev", None, None),
        P("tm", None, None),
        P(),
        P(),
    )
    return jax.shard_map(
        shards, mesh=mesh, in_specs=placed, out_specs=P(None, "lev", None, "tm"), check_vma=False
    )
```

```python
import functools
import math

import numpy as np

import jax
import jax.numpy as jnp
from jax import lax
from jax.experimental import pallas as pl
from jax.experimental.pallas import tpu as pltpu
from jax.sharding import PartitionSpec as P


LANES = 128
SUBLANES = 8
ACCUMULATORS = 8
OBS_BLOCK = 1024
INDEX_BUFFERS = 4
WAVE_UNROLL = 64
DEGREE_BLOCK = 16
TABLE_UNROLL = 8
SWEEP_MIB = 20


def vmem():
    return pl.BlockSpec(memory_space=pltpu.VMEM)


def in_hbm(*arrays):
    return [pltpu.with_memory_space_constraint(array, pltpu.HBM) for array in arrays]


def fourier_rows(lon_count, wave_count):
    longitude = np.arange(lon_count)[None, :]
    wavenumber = np.arange(wave_count)[:, None]
    angles = (longitude * wavenumber % lon_count) * (2.0 * math.pi / lon_count)
    rows = np.concatenate([np.cos(angles), np.sin(angles)]) * math.sqrt(2.0 / lon_count)
    rows = rows.astype(np.float32)
    high = rows.astype(jnp.bfloat16)
    low = (rows - high.astype(np.float32)).astype(jnp.bfloat16)
    return high, low


def legendre_seeds(lat_count, wave_count):
    orders = np.arange(wave_count, dtype=np.float64)[:, None]
    degrees = np.arange(wave_count, dtype=np.float64)[None, :]
    latitude = (np.arange(lat_count) + 0.5) * (math.pi / lat_count) - 0.5 * math.pi
    sine = np.sin(latitude)[None, :]
    cosine = np.cos(latitude)[None, :]
    gammas = np.array(
        [
            math.lgamma(order + 1.5) - math.lgamma(1.5) - math.lgamma(order + 1.0)
            for order in range(wave_count)
        ]
    )[:, None]
    diagonal = np.exp(-0.5 * math.log(2.0) + 0.5 * gammas + orders * np.log(cosine))
    diagonal = diagonal * np.sqrt(math.pi / lat_count * cosine)
    upward = np.sqrt(
        np.maximum(4.0 * degrees**2 - 1.0, 1.0) / np.maximum(degrees**2 - orders**2, 1.0)
    )
    lower = degrees - 1.0
    downward = np.sqrt(
        np.maximum(lower**2 - orders**2, 0.0) / np.maximum(4.0 * lower**2 - 1.0, 1.0)
    )
    sine = np.broadcast_to(sine, (SUBLANES, lat_count))
    return np.concatenate([upward, upward * downward, diagonal, sine]).astype(np.float32)


def split_parts(values):
    high = values.astype(jnp.bfloat16)
    low = (values - high.astype(jnp.float32)).astype(jnp.bfloat16)
    return high, low


def dot(left, right, left_dim, right_dim):
    return lax.dot_general(
        left, right, (((left_dim,), (right_dim,)), ((), ())), preferred_element_type=jnp.float32
    )


def legendre_kernel(
    seeds, fourier, spread, analysis, synthesis, fourier_near, spread_near, values, sems
):
    waves, lats = analysis.shape[:2]
    pitch = values.shape[0] // waves
    nearer = [
        pltpu.make_async_copy(fourier, fourier_near, sems.at[0]),
        pltpu.make_async_copy(spread, spread_near, sems.at[1]),
    ]
    for copy in nearer:
        copy.start()
    sine = seeds[3 * waves : 3 * waves + 1, :]
    one = jnp.zeros((0, lats), jnp.float32)
    two = one
    for degree in range(waves):
        live = (degree // DEGREE_BLOCK + 1) * DEGREE_BLOCK
        if one.shape[0] < live:
            fresh = jnp.zeros((live - one.shape[0], lats), jnp.float32)
            one = jnp.concatenate([one, fresh], axis=0) if one.shape[0] else fresh
            two = jnp.concatenate([two, fresh], axis=0) if two.shape[0] else fresh
        order = lax.broadcasted_iota(jnp.int32, (DEGREE_BLOCK, lats), 0) + (live - DEGREE_BLOCK)
        edge = slice(2 * waves + live - DEGREE_BLOCK, 2 * waves + live)
        seed = jnp.where(order == degree, seeds[edge, :], 0.0)
        if live > DEGREE_BLOCK:
            seed = jnp.concatenate(
                [jnp.zeros((live - DEGREE_BLOCK, lats), jnp.float32), seed], axis=0
            )
        up = seeds[0:live, degree : degree + 1]
        down = seeds[waves : waves + live, degree : degree + 1]
        current = (up * sine) * one - down * two + seed
        values[degree * pitch : degree * pitch + live, :] = current
        one, two = current, one

    row = lax.broadcasted_iota(jnp.int32, (lats, lats), 0)
    identity = (row == lax.broadcasted_iota(jnp.int32, (lats, lats), 1)).astype(jnp.bfloat16)
    for group in range(waves // DEGREE_BLOCK):
        skipped = group * DEGREE_BLOCK

        def emit(part, carry):
            for step in range(TABLE_UNROLL):
                wave = skipped + TABLE_UNROLL * part + step
                start = skipped * pitch + wave
                rows = values[pl.ds(start, waves - skipped, stride=pitch), :]
                if skipped:
                    rows = jnp.concatenate(
                        [jnp.zeros((skipped, lats), jnp.float32), rows], axis=0
                    )
                high, low = split_parts(rows)
                synthesis[wave] = jnp.concatenate([high, low], axis=1)
                if step % 2:
                    both = jnp.concatenate([high, low], axis=0)
                    analysis[wave] = dot(identity, both, 1, 1).astype(jnp.bfloat16)
                else:
                    analysis[wave] = jnp.concatenate(split_parts(rows.T), axis=1)
            return carry

        lax.fori_loop(0, DEGREE_BLOCK // TABLE_UNROLL, emit, 0)
    for copy in nearer:
        copy.wait()


def legendre_tables(lat_count, lon_count, wave_count, spread):
    pitch = wave_count + SUBLANES
    fourier = np.stack(fourier_rows(lon_count, wave_count))
    anywhere = pl.BlockSpec(memory_space=pl.ANY)
    return pl.pallas_call(
        legendre_kernel,
        out_shape=[
            jax.ShapeDtypeStruct((wave_count, lat_count, 2 * wave_count), jnp.bfloat16),
            jax.ShapeDtypeStruct((wave_count, wave_count, 2 * lat_count), jnp.bfloat16),
            jax.ShapeDtypeStruct(fourier.shape, jnp.bfloat16),
            jax.ShapeDtypeStruct(spread.shape, jnp.float32),
        ],
        in_specs=[vmem(), anywhere, anywhere],
        out_specs=[vmem()] * 4,
        scratch_shapes=[
            pltpu.VMEM((wave_count * pitch, lat_count), jnp.float32),
            pltpu.SemaphoreType.DMA((2,)),
        ],
        compiler_params=pltpu.CompilerParams(vmem_limit_bytes=14 * 2**20),
        name="legendre",
    )(*in_hbm(legendre_seeds(lat_count, wave_count), fourier, spread))


def scatter_kernel(rows, cells, innov, damping, *refs, sections, lats, lons):
    levels, obs = innov.shape
    outs = refs[:sections]
    field, sems = refs[sections : sections + 2]
    datas = refs[sections + 2 : sections + 4]
    nears = refs[sections + 4 : sections + 4 + INDEX_BUFFERS]
    near_sems = refs[sections + 4 + INDEX_BUFFERS]
    sums = refs[sections + 5 + INDEX_BUFFERS :]
    span = LANES // levels
    chunk = max(1, levels // sections)
    row = lax.broadcasted_iota(jnp.int32, (4 * SUBLANES, 2 * LANES), 0)
    lane = lax.broadcasted_iota(jnp.int32, (4 * SUBLANES, 2 * LANES), 1)
    values_here = (row < 3 * SUBLANES) & (lane < LANES) & (row % SUBLANES == lane // span)
    place = (values_here | ((row == 3 * SUBLANES) & (lane >= LANES))).astype(jnp.bfloat16)
    lane_low = (lax.broadcasted_iota(jnp.int32, (OBS_BLOCK, LANES), 1) % span).astype(jnp.float32)

    def spread_out(block, data):
        start = pl.multiple_of(block * OBS_BLOCK, OBS_BLOCK)
        rest = innov[:, pl.ds(start, OBS_BLOCK)]
        if levels < SUBLANES:
            fill = jnp.zeros((SUBLANES - levels, OBS_BLOCK), jnp.float32)
            rest = jnp.concatenate([rest, fill], axis=0)
        parts = []
        for _ in range(3):
            parts.append(rest.astype(jnp.bfloat16).astype(jnp.float32))
            rest = rest - parts[-1]
        low = (cells[:, pl.ds(start, OBS_BLOCK)] // lons % span).astype(jnp.float32)
        parts.append(jnp.broadcast_to(low, (SUBLANES, OBS_BLOCK)))
        stacked = jnp.concatenate(parts, axis=0).astype(jnp.bfloat16)
        placed = dot(stacked, place, 0, 0)
        data[...] = jnp.where(placed[:, LANES:] == lane_low, placed[:, :LANES], 0.0)

    def add_rows(near, data):
        for step in range(OBS_BLOCK):
            part = sums[step % ACCUMULATORS]
            at = pl.ds(near[step], 1)
            part[at, :] = part[at, :] + data[step : step + 1, :]

    def fetch(block, buffer):
        start = pl.multiple_of(block * OBS_BLOCK, OBS_BLOCK)
        return pltpu.make_async_copy(
            rows.at[pl.ds(start, OBS_BLOCK)], nears[buffer], near_sems.at[buffer]
        )

    blocks = obs // OBS_BLOCK
    for buffer in range(INDEX_BUFFERS):
        fetch(buffer, buffer).start()
    for part in sums:
        part[...] = jnp.zeros(part.shape, jnp.float32)
    spread_out(0, datas[0])

    def some_blocks(group, carry):
        for buffer in range(INDEX_BUFFERS):
            block = group * INDEX_BUFFERS + buffer
            fetch(block, buffer).wait()
            spread_out(jnp.minimum(block + 1, blocks - 1), datas[(buffer + 1) % 2])
            add_rows(nears[buffer], datas[buffer % 2])

            @pl.when(block + INDEX_BUFFERS < blocks)
            def _():
                fetch(block + INDEX_BUFFERS, buffer).start()

        return carry

    lax.fori_loop(0, blocks // INDEX_BUFFERS, some_blocks, 0)

    first = lax.axis_index("lev") * levels
    for high in range(lats // span):
        for west in range(lons // LANES):
            block = pl.ds(high * lons + west * LANES, LANES)
            total = sums[0][block, :]
            for part in sums[1:]:
                total = total + part[block, :]
            turned = total.T
            for k in range(levels):
                at = ((k % chunk) * (lons // LANES) + west) * lats + high * span
                field[k // chunk, at : at + span, :] = turned[k * span : (k + 1) * span, :]
    tail = chunk * lats * lons // LANES
    for piece in range(levels // chunk):
        field[piece, tail:, :] = jnp.zeros((SUBLANES, LANES), jnp.float32)
        for k in range(chunk):
            rates = damping[pl.ds(first + piece * chunk + k, 1), :]
            field[piece, tail + k : tail + k + 1, :] = rates
    me = lax.axis_index("tm")
    repeat = max(1, sections // levels)
    copies = [
        pltpu.make_async_copy(field.at[(me ^ slot) // repeat], outs[slot], sems.at[slot])
        for slot in range(sections)
    ]
    for copy in copies:
        copy.start()
    for copy in copies:
        copy.wait()


def cut_kernel(field, *refs, sections):
    outs, sems = refs[:sections], refs[sections]
    levels = field.shape[0]
    me = lax.axis_index("tm")
    chunk = max(1, levels // sections)
    repeat = max(1, sections // levels)
    copies = [
        pltpu.make_async_copy(
            field.at[pl.ds(((me ^ slot) // repeat) * chunk, chunk)], outs[slot], sems.at[slot]
        )
        for slot in range(sections)
    ]
    for copy in copies:
        copy.start()
    for copy in copies:
        copy.wait()


def cut_chunks(field, sections):
    levels, lats, lons = field.shape
    chunk = max(1, levels // sections)
    return pl.pallas_call(
        functools.partial(cut_kernel, sections=sections),
        out_shape=[jax.ShapeDtypeStruct((chunk, lats, lons), jnp.float32)] * sections,
        in_specs=[pl.BlockSpec(memory_space=pl.ANY)],
        out_specs=[vmem()] * sections,
        scratch_shapes=[pltpu.SemaphoreType.DMA((sections,))],
        compiler_params=pltpu.CompilerParams(vmem_limit_bytes=4 * 2**20),
        name="cut",
    )(field)


def forcing_chunks(cells, innov, damping, lats, lons, sections):
    levels, _ = innov.shape
    span = LANES // levels
    rows = (cells // (lons * span)) * lons + cells % lons
    chunk = max(1, levels // sections)
    size = chunk * lats * lons // LANES + SUBLANES
    return pl.pallas_call(
        functools.partial(scatter_kernel, sections=sections, lats=lats, lons=lons),
        out_shape=[jax.ShapeDtypeStruct((size, LANES), jnp.float32)] * sections,
        in_specs=[pl.BlockSpec(memory_space=pl.ANY), vmem(), vmem(), vmem()],
        out_specs=[pl.BlockSpec(memory_space=pl.ANY)] * sections,
        scratch_shapes=[
            pltpu.VMEM((levels // chunk, size, LANES), jnp.float32),
            pltpu.SemaphoreType.DMA((sections,)),
            pltpu.VMEM((OBS_BLOCK, LANES), jnp.float32),
            pltpu.VMEM((OBS_BLOCK, LANES), jnp.float32),
        ]
        + [pltpu.SMEM((OBS_BLOCK,), jnp.int32)] * INDEX_BUFFERS
        + [pltpu.SemaphoreType.DMA((INDEX_BUFFERS,))]
        + [pltpu.VMEM((lats * lons // span, LANES), jnp.float32)] * ACCUMULATORS,
        compiler_params=pltpu.CompilerParams(vmem_limit_bytes=32 * 2**20),
        name="scatter",
    )(rows, *in_hbm(cells[None, :], innov, damping))


def sweep_kernel(analysis, synthesis, fourier, spread, *refs, sections):
    chunks, tangents = refs[:sections], refs[sections : 2 * sections]
    out, forced, work, filtered, total, damp_now = refs[2 * sections :]
    fourier_high, fourier_low = fourier.at[0], fourier.at[1]
    waves, lats = analysis.shape[:2]
    times = sections
    degree_block = waves // times
    kept = tangents[0].shape[0]
    lons = tangents[0].shape[2]
    levels = spread.shape[0] // lax.axis_size("lev")
    half = 2 * kept
    rows = max(SUBLANES, 2 * half)
    copies = rows // half
    row = lax.broadcasted_iota(jnp.int32, (rows, waves), 0)
    is_high = (row // half) % 2 == 0
    total[...] = jnp.zeros(total.shape, jnp.float32)
    forced[...] = jnp.zeros(forced.shape, jnp.float32)
    me = lax.axis_index("tm")

    for time in range(times - 1, -1, -1):
        for slot in range(sections):

            @pl.when(me ^ slot == time)
            def _(chunk=chunks[slot]):
                for k in range(kept):
                    here = slice(k * lats, (k + 1) * lats)
                    for west in range(lons // LANES):
                        there = slice(west * LANES, (west + 1) * LANES)
                        at = (k * (lons // LANES) + west) * lats
                        forced[here, there] = forced[here, there] + chunk[at : at + lats, :]
                    tail = kept * lats * lons // LANES + k
                    damp_now[k : k + 1, :] = chunk[tail : tail + 1, :]

        high, low = split_parts(forced[...])
        coeffs = dot(fourier_high[...], high, 1, 1)
        coeffs = coeffs + dot(fourier_low[...], high, 1, 1)
        coeffs = coeffs + dot(fourier_high[...], low, 1, 1)
        for k in range(kept):
            for p in range(2):
                piece = coeffs[p * waves : (p + 1) * waves, k * lats : (k + 1) * lats]
                piece_high = piece.astype(jnp.bfloat16).astype(jnp.float32)
                piece_low = piece - piece_high
                for copy in range(copies):
                    at = copy * half + 2 * k + p
                    work[pl.ds(at, waves, stride=rows), :] = (
                        piece_high if copy % 2 == 0 else piece_low
                    )
        damp_rows = []
        for k in range(kept):
            damp_row = damp_now[k : k + 1, :]
            damp_rows += [damp_row, damp_row]
        damp = jnp.concatenate(damp_rows * copies, axis=0)

        def analyse(group, carry):
            for step in range(WAVE_UNROLL):
                wave = group * WAVE_UNROLL + step
                at = pl.ds(pl.multiple_of(wave * rows, rows), rows)
                product = dot(work[at, :].astype(jnp.bfloat16), analysis[wave], 1, 0)
                product = product[:, 0:waves] + product[:, waves:]
                spectral = product + pltpu.roll(product, half, 0)
                total[at, :] = total[at, :] + spectral
                if time > 0:
                    damped = spectral * damp
                    part = damped.astype(jnp.bfloat16).astype(jnp.float32)
                    filtered[at, :] = jnp.where(is_high, part, damped - part)
            return carry

        def synthesise(group, carry):
            for step in range(WAVE_UNROLL):
                wave = group * WAVE_UNROLL + step
                at = pl.ds(pl.multiple_of(wave * rows, rows), rows)
                result = dot(filtered[at, :].astype(jnp.bfloat16), synthesis[wave], 1, 0)
                result = result[:, 0:lats] + result[:, lats:]
                work[at, :] = result + pltpu.roll(result, half, 0)
            return carry

        lax.fori_loop(0, waves // WAVE_UNROLL, analyse, 0)
        if time > 0:
            for slot in range(sections):

                @pl.when(me ^ slot == time)
                def _(factor=tangents[slot]):
                    for k in range(kept):
                        here = slice(k * lats, (k + 1) * lats)
                        forced[here, :] = factor[k] * forced[here, :]

            lax.fori_loop(0, waves // WAVE_UNROLL, synthesise, 0)
            for k in range(kept):
                parts = [work[pl.ds(2 * k + p, waves, stride=rows), :].T for p in range(2)]
                synth_high, synth_low = split_parts(jnp.concatenate(parts, axis=1))
                gridded = dot(synth_high, fourier_high[...], 1, 0)
                gridded = gridded + dot(synth_high, fourier_low[...], 1, 0)
                gridded = gridded + dot(synth_low, fourier_high[...], 1, 0)
                here = slice(k * lats, (k + 1) * lats)
                forced[here, :] = forced[here, :] + gridded

    scaled = []
    repeat = max(1, sections // levels)
    first = lax.axis_index("lev") * levels + (me // repeat) * kept
    for k in range(kept):
        factor = spread[pl.ds(first + k, 1), :]
        for p in range(2):
            scaled.append(total[pl.ds(2 * k + p, waves, stride=rows), :] * factor)
    for block in range(times):
        cols = slice(block * degree_block, (block + 1) * degree_block)
        out[block] = jnp.concatenate([piece[:, cols] for piece in scaled], axis=1)


def sweep(chunks, tangents, tables):
    sections = len(chunks)
    kept, lats, lons = tangents[0].shape
    waves = tables[0].shape[0]
    rows = max(SUBLANES, 4 * kept)
    return pl.pallas_call(
        functools.partial(sweep_kernel, sections=sections),
        out_shape=jax.ShapeDtypeStruct(
            (sections, waves, 2 * kept * waves // sections), jnp.float32
        ),
        in_specs=[vmem()] * (4 + 2 * sections),
        out_specs=vmem(),
        scratch_shapes=[
            pltpu.VMEM((kept * lats, lons), jnp.float32),
            pltpu.VMEM((waves * rows, lats), jnp.float32),
            pltpu.VMEM((waves * rows, waves), jnp.float32),
            pltpu.VMEM((waves * rows, waves), jnp.float32),
            pltpu.VMEM((SUBLANES, waves), jnp.float32),
        ],
        compiler_params=pltpu.CompilerParams(vmem_limit_bytes=SWEEP_MIB * 2**20),
        name="sweep",
    )(*tables, *chunks, *tangents)


def mix_kernel(owned, vertical, out, *, sections, groups, repeat):
    peers = sections * groups
    block_waves = owned.shape[0] // peers
    lanes = owned.shape[1]
    steps = sections // repeat
    levels = vertical.shape[0] // groups
    kept = levels // steps
    each = lanes // kept
    columns = []
    for wave in range(block_waves):
        pieces = [
            owned[pl.ds(step * repeat * groups * block_waves + wave, groups, stride=block_waves), :]
            for step in range(steps)
        ]
        columns.append(jnp.concatenate(pieces, axis=0))
    high, low = split_parts(jnp.concatenate(columns, axis=1))
    left = jnp.concatenate([high, low, high], axis=0)
    for k in range(kept):
        pieces = [
            vertical[pl.ds(step * kept + k, groups, stride=levels), :] for step in range(steps)
        ]
        mix_high, mix_low = split_parts(jnp.concatenate(pieces, axis=0))
        product = dot(left, jnp.concatenate([mix_high, mix_high, mix_low], axis=0), 0, 0)
        for wave in range(block_waves):
            start = wave * lanes + k * each
            piece = product[start : start + each, :]
            out[wave] = piece if k == 0 else out[wave] + piece


def mix(owned, vertical, sections, groups, repeat):
    peers, block_waves, lanes = owned.shape
    steps = sections // repeat
    each = lanes // (vertical.shape[0] // groups // steps)
    return pl.pallas_call(
        functools.partial(mix_kernel, sections=sections, groups=groups, repeat=repeat),
        out_shape=jax.ShapeDtypeStruct((block_waves, each, vertical.shape[1]), jnp.float32),
        in_specs=[vmem()] * 2,
        out_specs=vmem(),
        compiler_params=pltpu.CompilerParams(vmem_limit_bytes=16 * 2**20),
        name="mix",
    )(owned.reshape(peers * block_waves, lanes), vertical)


def shards(obs_cell, innovation, tangent, damping, spread, vertical):
    sections = lax.axis_size("tm")
    groups = lax.axis_size("lev")
    lev_dev, lat_rows, lon_cols = tangent.shape[1:]
    wave_count = damping.shape[2]
    repeat = max(1, sections // lev_dev)
    kept = max(1, lev_dev // sections)

    def exchange(chunks):
        return [
            lax.ppermute(chunk, "tm", [(i, i ^ slot) for i in range(sections)]) if slot else chunk
            for slot, chunk in enumerate(chunks)
        ]

    cut = cut_chunks(*in_hbm(tangent[0]), sections)
    tangents = exchange(cut)
    chunks = forcing_chunks(obs_cell[0], innovation[0], damping[0], lat_rows, lon_cols, sections)
    chunks = exchange(chunks)
    tables = legendre_tables(lat_rows, lon_cols, wave_count, spread)
    blocks = sweep(chunks, tangents, tables)

    block_waves = wave_count // groups
    block_degrees = wave_count // sections
    blocks = blocks.reshape(sections * groups, block_waves, 2 * kept * block_degrees)
    owned = lax.all_to_all(blocks, ("tm", "lev"), split_axis=0, concat_axis=0, tiled=True)
    mixed = mix(owned, vertical, sections, groups, repeat)
    mixed = mixed.reshape(block_waves, 2, block_degrees, vertical.shape[1])
    return jnp.transpose(mixed, (3, 0, 1, 2))


def solution(mesh):
    placed = (
        P("tm", None),
        P("tm", "lev", None),
        P("tm", "lev", None, None),
        P("tm", None, None),
        P(),
        P(),
    )
    return jax.shard_map(
        shards, mesh=mesh, in_specs=placed, out_specs=P(None, "lev", None, "tm"), check_vma=False
    )
```

```python
import functools
import math

import numpy as np

import jax
import jax.numpy as jnp
from jax import lax
from jax.experimental import pallas as pl
from jax.experimental.pallas import tpu as pltpu
from jax.sharding import PartitionSpec as P


LANES = 128
SUBLANES = 8
ACCUMULATORS = 8
OBS_BLOCK = 1024
INDEX_BUFFERS = 4
WAVE_UNROLL = 64
DEGREE_BLOCK = 16
TABLE_UNROLL = 8
SWEEP_MIB = 20


def vmem():
    return pl.BlockSpec(memory_space=pltpu.VMEM)


def in_hbm(*arrays):
    return [pltpu.with_memory_space_constraint(array, pltpu.HBM) for array in arrays]


def fourier_rows(lon_count, wave_count):
    longitude = np.arange(lon_count)[None, :]
    wavenumber = np.arange(wave_count)[:, None]
    angles = (longitude * wavenumber % lon_count) * (2.0 * math.pi / lon_count)
    rows = np.concatenate([np.cos(angles), np.sin(angles)]) * math.sqrt(2.0 / lon_count)
    rows = rows.astype(np.float32)
    high = rows.astype(jnp.bfloat16)
    low = (rows - high.astype(np.float32)).astype(jnp.bfloat16)
    return high, low


def legendre_seeds(lat_count, wave_count):
    orders = np.arange(wave_count, dtype=np.float64)[:, None]
    degrees = np.arange(wave_count, dtype=np.float64)[None, :]
    latitude = (np.arange(lat_count) + 0.5) * (math.pi / lat_count) - 0.5 * math.pi
    sine = np.sin(latitude)[None, :]
    cosine = np.cos(latitude)[None, :]
    gammas = np.array(
        [
            math.lgamma(order + 1.5) - math.lgamma(1.5) - math.lgamma(order + 1.0)
            for order in range(wave_count)
        ]
    )[:, None]
    diagonal = np.exp(-0.5 * math.log(2.0) + 0.5 * gammas + orders * np.log(cosine))
    diagonal = diagonal * np.sqrt(math.pi / lat_count * cosine)
    upward = np.sqrt(
        np.maximum(4.0 * degrees**2 - 1.0, 1.0) / np.maximum(degrees**2 - orders**2, 1.0)
    )
    lower = degrees - 1.0
    downward = np.sqrt(
        np.maximum(lower**2 - orders**2, 0.0) / np.maximum(4.0 * lower**2 - 1.0, 1.0)
    )
    sine = np.broadcast_to(sine, (SUBLANES, lat_count))
    return np.concatenate([upward, upward * downward, diagonal, sine]).astype(np.float32)


def split_parts(values):
    high = values.astype(jnp.bfloat16)
    low = (values - high.astype(jnp.float32)).astype(jnp.bfloat16)
    return high, low


def dot(left, right, left_dim, right_dim):
    return lax.dot_general(
        left, right, (((left_dim,), (right_dim,)), ((), ())), preferred_element_type=jnp.float32
    )


def legendre_kernel(
    seeds, fourier, spread, analysis, synthesis, fourier_near, spread_near, values, sems
):
    waves, lats = analysis.shape[:2]
    pitch = values.shape[0] // waves
    nearer = [
        pltpu.make_async_copy(fourier, fourier_near, sems.at[0]),
        pltpu.make_async_copy(spread, spread_near, sems.at[1]),
    ]
    for copy in nearer:
        copy.start()
    sine = seeds[3 * waves : 3 * waves + 1, :]
    one = jnp.zeros((0, lats), jnp.float32)
    two = one
    for degree in range(waves):
        live = (degree // DEGREE_BLOCK + 1) * DEGREE_BLOCK
        if one.shape[0] < live:
            fresh = jnp.zeros((live - one.shape[0], lats), jnp.float32)
            one = jnp.concatenate([one, fresh], axis=0) if one.shape[0] else fresh
            two = jnp.concatenate([two, fresh], axis=0) if two.shape[0] else fresh
        order = lax.broadcasted_iota(jnp.int32, (DEGREE_BLOCK, lats), 0) + (live - DEGREE_BLOCK)
        edge = slice(2 * waves + live - DEGREE_BLOCK, 2 * waves + live)
        seed = jnp.where(order == degree, seeds[edge, :], 0.0)
        if live > DEGREE_BLOCK:
            seed = jnp.concatenate(
                [jnp.zeros((live - DEGREE_BLOCK, lats), jnp.float32), seed], axis=0
            )
        up = seeds[0:live, degree : degree + 1]
        down = seeds[waves : waves + live, degree : degree + 1]
        current = (up * sine) * one - down * two + seed
        values[degree * pitch : degree * pitch + live, :] = current
        one, two = current, one

    row = lax.broadcasted_iota(jnp.int32, (lats, lats), 0)
    identity = (row == lax.broadcasted_iota(jnp.int32, (lats, lats), 1)).astype(jnp.bfloat16)
    for group in range(waves // DEGREE_BLOCK):
        skipped = group * DEGREE_BLOCK

        def emit(part, carry):
            for step in range(TABLE_UNROLL):
                wave = skipped + TABLE_UNROLL * part + step
                start = skipped * pitch + wave
                rows = values[pl.ds(start, waves - skipped, stride=pitch), :]
                if skipped:
                    rows = jnp.concatenate(
                        [jnp.zeros((skipped, lats), jnp.float32), rows], axis=0
                    )
                high, low = split_parts(rows)
                synthesis[wave] = jnp.concatenate([high, low], axis=1)
                if step % 2:
                    both = jnp.concatenate([high, low], axis=0)
                    analysis[wave] = dot(identity, both, 1, 1).astype(jnp.bfloat16)
                else:
                    analysis[wave] = jnp.concatenate(split_parts(rows.T), axis=1)
            return carry

        lax.fori_loop(0, DEGREE_BLOCK // TABLE_UNROLL, emit, 0)
    for copy in nearer:
        copy.wait()


def legendre_tables(lat_count, lon_count, wave_count, spread):
    pitch = wave_count + SUBLANES
    fourier = np.stack(fourier_rows(lon_count, wave_count))
    anywhere = pl.BlockSpec(memory_space=pl.ANY)
    return pl.pallas_call(
        legendre_kernel,
        out_shape=[
            jax.ShapeDtypeStruct((wave_count, lat_count, 2 * wave_count), jnp.bfloat16),
            jax.ShapeDtypeStruct((wave_count, wave_count, 2 * lat_count), jnp.bfloat16),
            jax.ShapeDtypeStruct(fourier.shape, jnp.bfloat16),
            jax.ShapeDtypeStruct(spread.shape, jnp.float32),
        ],
        in_specs=[vmem(), anywhere, anywhere],
        out_specs=[vmem()] * 4,
        scratch_shapes=[
            pltpu.VMEM((wave_count * pitch, lat_count), jnp.float32),
            pltpu.SemaphoreType.DMA((2,)),
        ],
        compiler_params=pltpu.CompilerParams(vmem_limit_bytes=14 * 2**20),
        name="legendre",
    )(*in_hbm(legendre_seeds(lat_count, wave_count), fourier, spread))


def scatter_kernel(rows, cells, innov, damping, *refs, sections, slots, relayed, lats, lons):
    levels = innov.shape[0]
    obs = cells.shape[1]
    outs, refs = refs[:slots], refs[slots:]
    field, sems = refs[:2]
    datas = refs[2:4]
    nears = refs[4 : 4 + INDEX_BUFFERS]
    near_sems = refs[4 + INDEX_BUFFERS]
    sums = refs[5 + INDEX_BUFFERS :]
    span = LANES // levels
    chunk = max(1, levels // sections)
    row = lax.broadcasted_iota(jnp.int32, (4 * SUBLANES, 2 * LANES), 0)
    lane = lax.broadcasted_iota(jnp.int32, (4 * SUBLANES, 2 * LANES), 1)
    values_here = (row < 3 * SUBLANES) & (lane < LANES) & (row % SUBLANES == lane // span)
    place = (values_here | ((row == 3 * SUBLANES) & (lane >= LANES))).astype(jnp.bfloat16)
    lane_low = (lax.broadcasted_iota(jnp.int32, (OBS_BLOCK, LANES), 1) % span).astype(jnp.float32)

    def spread_out(block, data):
        start = pl.multiple_of(block * OBS_BLOCK, OBS_BLOCK)
        rest = innov[:, pl.ds(start, OBS_BLOCK)]
        if levels < SUBLANES:
            fill = jnp.zeros((SUBLANES - levels, OBS_BLOCK), jnp.float32)
            rest = jnp.concatenate([rest, fill], axis=0)
        parts = []
        for _ in range(3):
            parts.append(rest.astype(jnp.bfloat16).astype(jnp.float32))
            rest = rest - parts[-1]
        low = (cells[:, pl.ds(start, OBS_BLOCK)] // lons % span).astype(jnp.float32)
        parts.append(jnp.broadcast_to(low, (SUBLANES, OBS_BLOCK)))
        stacked = jnp.concatenate(parts, axis=0).astype(jnp.bfloat16)
        placed = dot(stacked, place, 0, 0)
        data[...] = jnp.where(placed[:, LANES:] == lane_low, placed[:, :LANES], 0.0)

    def add_rows(near, data):
        for step in range(OBS_BLOCK):
            part = sums[step % ACCUMULATORS]
            at = pl.ds(near[step], 1)
            part[at, :] = part[at, :] + data[step : step + 1, :]

    def fetch(block, buffer):
        start = pl.multiple_of(block * OBS_BLOCK, OBS_BLOCK)
        return pltpu.make_async_copy(
            rows.at[pl.ds(start, OBS_BLOCK)], nears[buffer], near_sems.at[buffer]
        )

    blocks = obs // OBS_BLOCK
    for buffer in range(INDEX_BUFFERS):
        fetch(buffer, buffer).start()
    for part in sums:
        part[...] = jnp.zeros(part.shape, jnp.float32)
    spread_out(0, datas[0])

    def some_blocks(group, carry):
        for buffer in range(INDEX_BUFFERS):
            block = group * INDEX_BUFFERS + buffer
            fetch(block, buffer).wait()
            spread_out(jnp.minimum(block + 1, blocks - 1), datas[(buffer + 1) % 2])
            add_rows(nears[buffer], datas[buffer % 2])

            @pl.when(block + INDEX_BUFFERS < blocks)
            def _():
                fetch(block + INDEX_BUFFERS, buffer).start()

        return carry

    lax.fori_loop(0, blocks // INDEX_BUFFERS, some_blocks, 0)

    first = lax.axis_index("lev") * levels
    for high in range(lats // span):
        for west in range(lons // LANES):
            block = pl.ds(high * lons + west * LANES, LANES)
            total = sums[0][block, :]
            for part in sums[1:]:
                total = total + part[block, :]
            turned = total.T
            for k in range(levels):
                at = ((k % chunk) * (lons // LANES) + west) * lats + high * span
                field[k // chunk, at : at + span, :] = turned[k * span : (k + 1) * span, :]
    tail = chunk * lats * lons // LANES
    for piece in range(levels // chunk):
        field[piece, tail:, :] = jnp.zeros((SUBLANES, LANES), jnp.float32)
        for k in range(chunk):
            if relayed:
                rates = innov[k : k + 1, obs:]
            else:
                rates = damping[pl.ds(first + piece * chunk + k, 1), :]
            field[piece, tail + k : tail + k + 1, :] = rates
    me = lax.axis_index("tm")
    repeat = max(1, sections // levels)
    pieces = levels // chunk
    copies = [
        pltpu.make_async_copy(field.at[(me ^ slot) // repeat % pieces], outs[slot], sems.at[slot])
        for slot in range(slots)
    ]
    for copy in copies:
        copy.start()
    for copy in copies:
        copy.wait()


def cut_kernel(field, innov, damping, *refs, sections, relayed):
    outs, refs = refs[:sections], refs[sections:]
    levels = field.shape[0]
    me = lax.axis_index("tm")
    chunk = max(1, levels // sections)
    repeat = max(1, sections // levels)
    sems = refs[-1]
    copies = [
        pltpu.make_async_copy(
            field.at[pl.ds(((me ^ slot) // repeat) * chunk, chunk)], outs[slot], sems.at[slot]
        )
        for slot in range(sections)
    ]
    if relayed:
        relay, innov_near, damping_near = refs[:3]
        nearer = [
            pltpu.make_async_copy(innov, innov_near, sems.at[sections]),
            pltpu.make_async_copy(damping, damping_near, sems.at[sections + 1]),
        ]
        copies = nearer + copies
    for copy in copies:
        copy.start()
    if relayed:
        for copy in nearer:
            copy.wait()
        obs = innov.shape[1]
        first = lax.axis_index("lev") * levels + (me ^ relayed) * chunk
        for k in range(chunk):
            relay[k : k + 1, obs:] = damping_near[pl.ds(first + k, 1), :]
        for piece in range(sections):

            @pl.when(me ^ relayed == piece)
            def _(here=slice(piece * chunk, (piece + 1) * chunk)):
                relay[:, 0:obs] = innov_near[here, :]

        copies = copies[2:]
    for copy in copies:
        copy.wait()


def cut_chunks(field, innov, damping, sections, relayed):
    levels, lats, lons = field.shape
    chunk = max(1, levels // sections)
    out_shape = [jax.ShapeDtypeStruct((chunk, lats, lons), jnp.float32)] * sections
    scratch = []
    if relayed:
        width = innov.shape[1] + damping.shape[1]
        out_shape = out_shape + [jax.ShapeDtypeStruct((chunk, width), jnp.float32)]
        scratch = [pltpu.VMEM(innov.shape, jnp.float32), pltpu.VMEM(damping.shape, jnp.float32)]
    return pl.pallas_call(
        functools.partial(cut_kernel, sections=sections, relayed=relayed),
        out_shape=out_shape,
        in_specs=[pl.BlockSpec(memory_space=pl.ANY)] * 3,
        out_specs=[vmem()] * len(out_shape),
        scratch_shapes=scratch + [pltpu.SemaphoreType.DMA((sections + 2,))],
        compiler_params=pltpu.CompilerParams(vmem_limit_bytes=6 * 2**20),
        name="cut",
    )(*in_hbm(field, innov, damping))


def forcing_chunks(cells, innov, damping, lats, lons, sections, slots, relayed=False):
    levels = innov.shape[0]
    span = LANES // levels
    rows = (cells // (lons * span)) * lons + cells % lons
    inputs = (cells[None, :], innov, damping)
    chunk = max(1, levels // sections)
    size = chunk * lats * lons // LANES + SUBLANES
    return pl.pallas_call(
        functools.partial(
            scatter_kernel,
            sections=sections,
            slots=slots,
            relayed=relayed,
            lats=lats,
            lons=lons,
        ),
        out_shape=[jax.ShapeDtypeStruct((size, LANES), jnp.float32)] * slots,
        in_specs=[pl.BlockSpec(memory_space=pl.ANY), vmem(), vmem(), vmem()],
        out_specs=[pl.BlockSpec(memory_space=pl.ANY)] * slots,
        scratch_shapes=[
            pltpu.VMEM((levels // chunk, size, LANES), jnp.float32),
            pltpu.SemaphoreType.DMA((slots,)),
            pltpu.VMEM((OBS_BLOCK, LANES), jnp.float32),
            pltpu.VMEM((OBS_BLOCK, LANES), jnp.float32),
        ]
        + [pltpu.SMEM((OBS_BLOCK,), jnp.int32)] * INDEX_BUFFERS
        + [pltpu.SemaphoreType.DMA((INDEX_BUFFERS,))]
        + [pltpu.VMEM((lats * lons // span, LANES), jnp.float32)] * ACCUMULATORS,
        compiler_params=pltpu.CompilerParams(vmem_limit_bytes=(12 if relayed else 32) * 2**20),
        name="scatter",
    )(rows, *(inputs if relayed else in_hbm(*inputs)))


def sweep_kernel(analysis, synthesis, fourier, spread, *refs, sections):
    chunks, tangents = refs[:sections], refs[sections : 2 * sections]
    out, forced, work, filtered, total, damp_now = refs[2 * sections :]
    fourier_high, fourier_low = fourier.at[0], fourier.at[1]
    waves, lats = analysis.shape[:2]
    times = sections
    degree_block = waves // times
    kept = tangents[0].shape[0]
    lons = tangents[0].shape[2]
    levels = spread.shape[0] // lax.axis_size("lev")
    half = 2 * kept
    rows = max(SUBLANES, 2 * half)
    copies = rows // half
    row = lax.broadcasted_iota(jnp.int32, (rows, waves), 0)
    is_high = (row // half) % 2 == 0
    total[...] = jnp.zeros(total.shape, jnp.float32)
    forced[...] = jnp.zeros(forced.shape, jnp.float32)
    me = lax.axis_index("tm")

    for time in range(times - 1, -1, -1):
        for slot in range(sections):

            @pl.when(me ^ slot == time)
            def _(chunk=chunks[slot]):
                for k in range(kept):
                    here = slice(k * lats, (k + 1) * lats)
                    for west in range(lons // LANES):
                        there = slice(west * LANES, (west + 1) * LANES)
                        at = (k * (lons // LANES) + west) * lats
                        forced[here, there] = forced[here, there] + chunk[at : at + lats, :]
                    tail = kept * lats * lons // LANES + k
                    damp_now[k : k + 1, :] = chunk[tail : tail + 1, :]

        high, low = split_parts(forced[...])
        coeffs = dot(fourier_high[...], high, 1, 1)
        coeffs = coeffs + dot(fourier_low[...], high, 1, 1)
        coeffs = coeffs + dot(fourier_high[...], low, 1, 1)
        for k in range(kept):
            for p in range(2):
                piece = coeffs[p * waves : (p + 1) * waves, k * lats : (k + 1) * lats]
                piece_high = piece.astype(jnp.bfloat16).astype(jnp.float32)
                piece_low = piece - piece_high
                for copy in range(copies):
                    at = copy * half + 2 * k + p
                    work[pl.ds(at, waves, stride=rows), :] = (
                        piece_high if copy % 2 == 0 else piece_low
                    )
        damp_rows = []
        for k in range(kept):
            damp_row = damp_now[k : k + 1, :]
            damp_rows += [damp_row, damp_row]
        damp = jnp.concatenate(damp_rows * copies, axis=0)

        def analyse(group, carry):
            for step in range(WAVE_UNROLL):
                wave = group * WAVE_UNROLL + step
                at = pl.ds(pl.multiple_of(wave * rows, rows), rows)
                product = dot(work[at, :].astype(jnp.bfloat16), analysis[wave], 1, 0)
                product = product[:, 0:waves] + product[:, waves:]
                spectral = product + pltpu.roll(product, half, 0)
                total[at, :] = total[at, :] + spectral
                if time > 0:
                    damped = spectral * damp
                    part = damped.astype(jnp.bfloat16).astype(jnp.float32)
                    filtered[at, :] = jnp.where(is_high, part, damped - part)
            return carry

        def synthesise(group, carry):
            for step in range(WAVE_UNROLL):
                wave = group * WAVE_UNROLL + step
                at = pl.ds(pl.multiple_of(wave * rows, rows), rows)
                result = dot(filtered[at, :].astype(jnp.bfloat16), synthesis[wave], 1, 0)
                result = result[:, 0:lats] + result[:, lats:]
                work[at, :] = result + pltpu.roll(result, half, 0)
            return carry

        lax.fori_loop(0, waves // WAVE_UNROLL, analyse, 0)
        if time > 0:
            for slot in range(sections):

                @pl.when(me ^ slot == time)
                def _(factor=tangents[slot]):
                    for k in range(kept):
                        here = slice(k * lats, (k + 1) * lats)
                        forced[here, :] = factor[k] * forced[here, :]

            lax.fori_loop(0, waves // WAVE_UNROLL, synthesise, 0)
            for k in range(kept):
                parts = [work[pl.ds(2 * k + p, waves, stride=rows), :].T for p in range(2)]
                synth_high, synth_low = split_parts(jnp.concatenate(parts, axis=1))
                gridded = dot(synth_high, fourier_high[...], 1, 0)
                gridded = gridded + dot(synth_high, fourier_low[...], 1, 0)
                gridded = gridded + dot(synth_low, fourier_high[...], 1, 0)
                here = slice(k * lats, (k + 1) * lats)
                forced[here, :] = forced[here, :] + gridded

    scaled = []
    repeat = max(1, sections // levels)
    first = lax.axis_index("lev") * levels + (me // repeat) * kept
    for k in range(kept):
        factor = spread[pl.ds(first + k, 1), :]
        for p in range(2):
            scaled.append(total[pl.ds(2 * k + p, waves, stride=rows), :] * factor)
    for block in range(times):
        cols = slice(block * degree_block, (block + 1) * degree_block)
        out[block] = jnp.concatenate([piece[:, cols] for piece in scaled], axis=1)


def sweep(chunks, tangents, tables):
    sections = len(chunks)
    kept, lats, lons = tangents[0].shape
    waves = tables[0].shape[0]
    rows = max(SUBLANES, 4 * kept)
    return pl.pallas_call(
        functools.partial(sweep_kernel, sections=sections),
        out_shape=jax.ShapeDtypeStruct(
            (sections, waves, 2 * kept * waves // sections), jnp.float32
        ),
        in_specs=[vmem()] * (4 + 2 * sections),
        out_specs=vmem(),
        scratch_shapes=[
            pltpu.VMEM((kept * lats, lons), jnp.float32),
            pltpu.VMEM((waves * rows, lats), jnp.float32),
            pltpu.VMEM((waves * rows, waves), jnp.float32),
            pltpu.VMEM((waves * rows, waves), jnp.float32),
            pltpu.VMEM((SUBLANES, waves), jnp.float32),
        ],
        compiler_params=pltpu.CompilerParams(vmem_limit_bytes=SWEEP_MIB * 2**20),
        name="sweep",
    )(*tables, *chunks, *tangents)


def mix_kernel(owned, vertical, out, *, sections, groups, repeat):
    peers = sections * groups
    block_waves = owned.shape[0] // peers
    lanes = owned.shape[1]
    steps = sections // repeat
    levels = vertical.shape[0] // groups
    kept = levels // steps
    each = lanes // kept
    columns = []
    for wave in range(block_waves):
        pieces = [
            owned[pl.ds(step * repeat * groups * block_waves + wave, groups, stride=block_waves), :]
            for step in range(steps)
        ]
        columns.append(jnp.concatenate(pieces, axis=0))
    high, low = split_parts(jnp.concatenate(columns, axis=1))
    left = jnp.concatenate([high, low, high], axis=0)
    for k in range(kept):
        pieces = [
            vertical[pl.ds(step * kept + k, groups, stride=levels), :] for step in range(steps)
        ]
        mix_high, mix_low = split_parts(jnp.concatenate(pieces, axis=0))
        product = dot(left, jnp.concatenate([mix_high, mix_high, mix_low], axis=0), 0, 0)
        for wave in range(block_waves):
            start = wave * lanes + k * each
            piece = product[start : start + each, :]
            out[wave] = piece if k == 0 else out[wave] + piece


def mix(owned, vertical, sections, groups, repeat):
    peers, block_waves, lanes = owned.shape
    steps = sections // repeat
    each = lanes // (vertical.shape[0] // groups // steps)
    return pl.pallas_call(
        functools.partial(mix_kernel, sections=sections, groups=groups, repeat=repeat),
        out_shape=jax.ShapeDtypeStruct((block_waves, each, vertical.shape[1]), jnp.float32),
        in_specs=[vmem()] * 2,
        out_specs=vmem(),
        compiler_params=pltpu.CompilerParams(vmem_limit_bytes=16 * 2**20),
        name="mix",
    )(owned.reshape(peers * block_waves, lanes), vertical)


def shards(obs_cell, innovation, tangent, damping, spread, vertical):
    sections = lax.axis_size("tm")
    groups = lax.axis_size("lev")
    lev_dev, lat_rows, lon_cols = tangent.shape[1:]
    wave_count = damping.shape[2]
    repeat = max(1, sections // lev_dev)
    kept = max(1, lev_dev // sections)

    relayed = sections - 1 if lev_dev >= sections > 2 else 0
    direct = relayed or sections

    def send(value, slot):
        return lax.ppermute(value, "tm", [(i, i ^ slot) for i in range(sections)])

    def exchange(chunks):
        return [send(chunk, slot) if slot else chunk for slot, chunk in enumerate(chunks)]

    cells, innov, rates = obs_cell[0], innovation[0], damping[0]
    cut = cut_chunks(tangent[0], innov, rates, sections, relayed)
    if relayed:
        far = send(cut[sections], relayed)
        far_cells = send(obs_cell, relayed)[0]
    tangents = exchange(cut[:sections])
    chunks = forcing_chunks(
        cells, innov, rates, lat_rows, lon_cols, sections, direct
    )
    chunks = exchange(chunks)
    if relayed:
        chunks += forcing_chunks(far_cells, far, rates, lat_rows, lon_cols, 1, 1, True)
    tables = legendre_tables(lat_rows, lon_cols, wave_count, spread)
    blocks = sweep(chunks, tangents, tables)

    block_waves = wave_count // groups
    block_degrees = wave_count // sections
    blocks = blocks.reshape(sections * groups, block_waves, 2 * kept * block_degrees)
    owned = lax.all_to_all(blocks, ("tm", "lev"), split_axis=0, concat_axis=0, tiled=True)
    mixed = mix(owned, vertical, sections, groups, repeat)
    mixed = mixed.reshape(block_waves, 2, block_degrees, vertical.shape[1])
    return jnp.transpose(mixed, (3, 0, 1, 2))


def solution(mesh):
    placed = (
        P("tm", None),
        P("tm", "lev", None),
        P("tm", "lev", None, None),
        P("tm", None, None),
        P(),
        P(),
    )
    return jax.shard_map(
        shards, mesh=mesh, in_specs=placed, out_specs=P(None, "lev", None, "tm"), check_vma=False
    )
```

```python
import functools
import math

import numpy as np

import jax
import jax.numpy as jnp
from jax import lax
from jax.experimental import pallas as pl
from jax.experimental.pallas import tpu as pltpu
from jax.sharding import PartitionSpec as P


LANES = 128
SUBLANES = 8
ACCUMULATORS = 8
OBS_BLOCK = 1024
INDEX_BUFFERS = 4
WAVE_UNROLL = 64
DEGREE_BLOCK = 16
TABLE_UNROLL = 8
SWEEP_MIB = 20


def vmem():
    return pl.BlockSpec(memory_space=pltpu.VMEM)


def in_hbm(*arrays):
    return [pltpu.with_memory_space_constraint(array, pltpu.HBM) for array in arrays]


def fourier_rows(lon_count, wave_count):
    longitude = np.arange(lon_count)[None, :]
    wavenumber = np.arange(wave_count)[:, None]
    angles = (longitude * wavenumber % lon_count) * (2.0 * math.pi / lon_count)
    rows = np.concatenate([np.cos(angles), np.sin(angles)]) * math.sqrt(2.0 / lon_count)
    rows = rows.astype(np.float32)
    high = rows.astype(jnp.bfloat16)
    low = (rows - high.astype(np.float32)).astype(jnp.bfloat16)
    return high, low


def legendre_seeds(lat_count, wave_count):
    orders = np.arange(wave_count, dtype=np.float64)[:, None]
    degrees = np.arange(wave_count, dtype=np.float64)[None, :]
    latitude = (np.arange(lat_count) + 0.5) * (math.pi / lat_count) - 0.5 * math.pi
    sine = np.sin(latitude)[None, :]
    cosine = np.cos(latitude)[None, :]
    gammas = np.array(
        [
            math.lgamma(order + 1.5) - math.lgamma(1.5) - math.lgamma(order + 1.0)
            for order in range(wave_count)
        ]
    )[:, None]
    diagonal = np.exp(-0.5 * math.log(2.0) + 0.5 * gammas + orders * np.log(cosine))
    diagonal = diagonal * np.sqrt(math.pi / lat_count * cosine)
    upward = np.sqrt(
        np.maximum(4.0 * degrees**2 - 1.0, 1.0) / np.maximum(degrees**2 - orders**2, 1.0)
    )
    lower = degrees - 1.0
    downward = np.sqrt(
        np.maximum(lower**2 - orders**2, 0.0) / np.maximum(4.0 * lower**2 - 1.0, 1.0)
    )
    sine = np.broadcast_to(sine, (SUBLANES, lat_count))
    return np.concatenate([upward, upward * downward, diagonal, sine]).astype(np.float32)


def split_parts(values):
    high = values.astype(jnp.bfloat16)
    low = (values - high.astype(jnp.float32)).astype(jnp.bfloat16)
    return high, low


def dot(left, right, left_dim, right_dim):
    return lax.dot_general(
        left, right, (((left_dim,), (right_dim,)), ((), ())), preferred_element_type=jnp.float32
    )


def bring_near(fourier, spread, fourier_near, spread_near, sems):
    return [
        pltpu.make_async_copy(fourier, fourier_near, sems.at[0]),
        pltpu.make_async_copy(spread, spread_near, sems.at[1]),
    ]


def legendre_values(seeds, values, fill):
    lats = values.shape[1]
    waves = seeds.shape[0] // 3 // DEGREE_BLOCK * DEGREE_BLOCK
    pitch = values.shape[0] // waves
    sine = seeds[3 * waves : 3 * waves + 1, :]
    one = jnp.zeros((0, lats), jnp.float32)
    two = one
    for degree in range(waves):
        live = (degree // DEGREE_BLOCK + 1) * DEGREE_BLOCK
        if one.shape[0] < live:
            fresh = jnp.zeros((live - one.shape[0], lats), jnp.float32)
            one = jnp.concatenate([one, fresh], axis=0) if one.shape[0] else fresh
            two = jnp.concatenate([two, fresh], axis=0) if two.shape[0] else fresh
        order = lax.broadcasted_iota(jnp.int32, (DEGREE_BLOCK, lats), 0) + (live - DEGREE_BLOCK)
        edge = slice(2 * waves + live - DEGREE_BLOCK, 2 * waves + live)
        seed = jnp.where(order == degree, seeds[edge, :], 0.0)
        if live > DEGREE_BLOCK:
            seed = jnp.concatenate(
                [jnp.zeros((live - DEGREE_BLOCK, lats), jnp.float32), seed], axis=0
            )
        up = seeds[0:live, degree : degree + 1]
        down = seeds[waves : waves + live, degree : degree + 1]
        current = (up * sine) * one - down * two + seed
        values[degree * pitch : degree * pitch + live, :] = current
        if fill and live < waves:
            values[degree * pitch + live : degree * pitch + waves, :] = jnp.zeros(
                (waves - live, lats), jnp.float32
            )
        one, two = current, one


def write_tables(values, analysis, synthesis, wave, skipped, turn):
    waves, lats = analysis.shape[:2]
    pitch = values.shape[0] // waves
    start = skipped * pitch + wave
    rows = values[pl.ds(start, waves - skipped, stride=pitch), :]
    if skipped:
        rows = jnp.concatenate([jnp.zeros((skipped, lats), jnp.float32), rows], axis=0)
    high, low = split_parts(rows)
    synthesis[wave] = jnp.concatenate([high, low], axis=1)
    if turn:
        row = lax.broadcasted_iota(jnp.int32, (lats, lats), 0)
        column = lax.broadcasted_iota(jnp.int32, (lats, lats), 1)
        identity = (row == column).astype(jnp.bfloat16)
        both = jnp.concatenate([high, low], axis=0)
        analysis[wave] = dot(identity, both, 1, 1).astype(jnp.bfloat16)
    else:
        analysis[wave] = jnp.concatenate(split_parts(rows.T), axis=1)


def legendre_kernel(
    seeds, fourier, spread, analysis, synthesis, fourier_near, spread_near, values, sems
):
    waves = analysis.shape[0]
    nearer = bring_near(fourier, spread, fourier_near, spread_near, sems)
    for copy in nearer:
        copy.start()
    legendre_values(seeds, values, False)
    for group in range(waves // DEGREE_BLOCK):
        skipped = group * DEGREE_BLOCK

        def emit(part, carry):
            for step in range(TABLE_UNROLL):
                wave = skipped + TABLE_UNROLL * part + step
                write_tables(values, analysis, synthesis, wave, skipped, step % 2)
            return carry

        lax.fori_loop(0, DEGREE_BLOCK // TABLE_UNROLL, emit, 0)
    for copy in nearer:
        copy.wait()


def far_kernel(
    rows,
    cells,
    innov,
    damping,
    seeds,
    fourier,
    spread,
    chunk,
    analysis,
    synthesis,
    fourier_near,
    spread_near,
    values,
    near_sems,
    *scratch,
    lats,
    lons,
):
    nearer = bring_near(fourier, spread, fourier_near, spread_near, near_sems)
    for copy in nearer:
        copy.start()
    legendre_values(seeds, values, True)
    each = analysis.shape[0] // (cells.shape[1] // OBS_BLOCK)

    def some_tables(block):
        for step in range(each):
            write_tables(values, analysis, synthesis, block * each + step, 0, step % 2)

    scatter_kernel(
        rows,
        cells,
        innov,
        damping,
        chunk,
        *scratch,
        sections=1,
        slots=1,
        relayed=True,
        lats=lats,
        lons=lons,
        beside=some_tables,
    )
    for copy in nearer:
        copy.wait()


def table_shapes(lats, waves, fourier, spread):
    return [
        jax.ShapeDtypeStruct((waves, lats, 2 * waves), jnp.bfloat16),
        jax.ShapeDtypeStruct((waves, waves, 2 * lats), jnp.bfloat16),
        jax.ShapeDtypeStruct(fourier.shape, jnp.bfloat16),
        jax.ShapeDtypeStruct(spread.shape, jnp.float32),
    ]


def far_chunk_and_tables(cells, innov, damping, lats, lons, waves, spread):
    levels = innov.shape[0]
    span = LANES // levels
    rows = (cells // (lons * span)) * lons + cells % lons
    size = levels * lats * lons // LANES + SUBLANES
    fourier = np.stack(fourier_rows(lons, waves))
    anywhere = pl.BlockSpec(memory_space=pl.ANY)
    far = in_hbm(damping, legendre_seeds(lats, waves), fourier, spread)
    chunk, *tables = pl.pallas_call(
        functools.partial(far_kernel, lats=lats, lons=lons),
        out_shape=[jax.ShapeDtypeStruct((size, LANES), jnp.float32)]
        + table_shapes(lats, waves, fourier, spread),
        in_specs=[anywhere, vmem(), vmem(), anywhere, vmem(), anywhere, anywhere],
        out_specs=[anywhere] + [vmem()] * 4,
        scratch_shapes=[
            pltpu.VMEM((waves * (waves + SUBLANES), lats), jnp.float32),
            pltpu.SemaphoreType.DMA((2,)),
        ]
        + scatter_scratch(levels, levels, size, 1, lats * lons // span),
        compiler_params=pltpu.CompilerParams(vmem_limit_bytes=24 * 2**20),
        name="far",
    )(rows, cells[None, :], innov, *far)
    return chunk, tables


def legendre_tables(lat_count, lon_count, wave_count, spread):
    pitch = wave_count + SUBLANES
    fourier = np.stack(fourier_rows(lon_count, wave_count))
    anywhere = pl.BlockSpec(memory_space=pl.ANY)
    return pl.pallas_call(
        legendre_kernel,
        out_shape=table_shapes(lat_count, wave_count, fourier, spread),
        in_specs=[vmem(), anywhere, anywhere],
        out_specs=[vmem()] * 4,
        scratch_shapes=[
            pltpu.VMEM((wave_count * pitch, lat_count), jnp.float32),
            pltpu.SemaphoreType.DMA((2,)),
        ],
        compiler_params=pltpu.CompilerParams(vmem_limit_bytes=14 * 2**20),
        name="legendre",
    )(*in_hbm(legendre_seeds(lat_count, wave_count), fourier, spread))


def scatter_kernel(
    rows, cells, innov, damping, *refs, sections, slots, relayed, lats, lons, beside=None
):
    levels = innov.shape[0]
    obs = cells.shape[1]
    outs, refs = refs[:slots], refs[slots:]
    field, sems = refs[:2]
    datas = refs[2:4]
    nears = refs[4 : 4 + INDEX_BUFFERS]
    near_sems = refs[4 + INDEX_BUFFERS]
    sums = refs[5 + INDEX_BUFFERS :]
    span = LANES // levels
    chunk = max(1, levels // sections)
    row = lax.broadcasted_iota(jnp.int32, (4 * SUBLANES, 2 * LANES), 0)
    lane = lax.broadcasted_iota(jnp.int32, (4 * SUBLANES, 2 * LANES), 1)
    values_here = (row < 3 * SUBLANES) & (lane < LANES) & (row % SUBLANES == lane // span)
    place = (values_here | ((row == 3 * SUBLANES) & (lane >= LANES))).astype(jnp.bfloat16)
    lane_low = (lax.broadcasted_iota(jnp.int32, (OBS_BLOCK, LANES), 1) % span).astype(jnp.float32)

    def spread_out(block, data):
        start = pl.multiple_of(block * OBS_BLOCK, OBS_BLOCK)
        rest = innov[:, pl.ds(start, OBS_BLOCK)]
        if levels < SUBLANES:
            fill = jnp.zeros((SUBLANES - levels, OBS_BLOCK), jnp.float32)
            rest = jnp.concatenate([rest, fill], axis=0)
        parts = []
        for _ in range(3):
            parts.append(rest.astype(jnp.bfloat16).astype(jnp.float32))
            rest = rest - parts[-1]
        low = (cells[:, pl.ds(start, OBS_BLOCK)] // lons % span).astype(jnp.float32)
        parts.append(jnp.broadcast_to(low, (SUBLANES, OBS_BLOCK)))
        stacked = jnp.concatenate(parts, axis=0).astype(jnp.bfloat16)
        placed = dot(stacked, place, 0, 0)
        data[...] = jnp.where(placed[:, LANES:] == lane_low, placed[:, :LANES], 0.0)

    def add_rows(near, data):
        for step in range(OBS_BLOCK):
            part = sums[step % ACCUMULATORS]
            at = pl.ds(near[step], 1)
            part[at, :] = part[at, :] + data[step : step + 1, :]

    def fetch(block, buffer):
        start = pl.multiple_of(block * OBS_BLOCK, OBS_BLOCK)
        return pltpu.make_async_copy(
            rows.at[pl.ds(start, OBS_BLOCK)], nears[buffer], near_sems.at[buffer]
        )

    blocks = obs // OBS_BLOCK
    for buffer in range(INDEX_BUFFERS):
        fetch(buffer, buffer).start()
    for part in sums:
        part[...] = jnp.zeros(part.shape, jnp.float32)
    spread_out(0, datas[0])

    def some_blocks(group, carry):
        for buffer in range(INDEX_BUFFERS):
            block = group * INDEX_BUFFERS + buffer
            fetch(block, buffer).wait()
            spread_out(jnp.minimum(block + 1, blocks - 1), datas[(buffer + 1) % 2])
            if beside:
                beside(block)
            add_rows(nears[buffer], datas[buffer % 2])

            @pl.when(block + INDEX_BUFFERS < blocks)
            def _():
                fetch(block + INDEX_BUFFERS, buffer).start()

        return carry

    lax.fori_loop(0, blocks // INDEX_BUFFERS, some_blocks, 0)

    first = lax.axis_index("lev") * levels
    for high in range(lats // span):
        for west in range(lons // LANES):
            block = pl.ds(high * lons + west * LANES, LANES)
            total = sums[0][block, :]
            for part in sums[1:]:
                total = total + part[block, :]
            turned = total.T
            for k in range(levels):
                at = ((k % chunk) * (lons // LANES) + west) * lats + high * span
                field[k // chunk, at : at + span, :] = turned[k * span : (k + 1) * span, :]
    tail = chunk * lats * lons // LANES
    for piece in range(levels // chunk):
        field[piece, tail:, :] = jnp.zeros((SUBLANES, LANES), jnp.float32)
        for k in range(chunk):
            if relayed:
                rates = innov[k : k + 1, obs:]
            else:
                rates = damping[pl.ds(first + piece * chunk + k, 1), :]
            field[piece, tail + k : tail + k + 1, :] = rates
    me = lax.axis_index("tm")
    repeat = max(1, sections // levels)
    pieces = levels // chunk
    copies = [
        pltpu.make_async_copy(field.at[(me ^ slot) // repeat % pieces], outs[slot], sems.at[slot])
        for slot in range(slots)
    ]
    for copy in copies:
        copy.start()
    for copy in copies:
        copy.wait()


def cut_kernel(field, innov, damping, *refs, sections, relayed):
    outs, refs = refs[:sections], refs[sections:]
    levels = field.shape[0]
    me = lax.axis_index("tm")
    chunk = max(1, levels // sections)
    repeat = max(1, sections // levels)
    sems = refs[-1]
    copies = [
        pltpu.make_async_copy(
            field.at[pl.ds(((me ^ slot) // repeat) * chunk, chunk)], outs[slot], sems.at[slot]
        )
        for slot in range(sections)
    ]
    if relayed:
        relay, innov_near, damping_near = refs[:3]
        nearer = [
            pltpu.make_async_copy(innov, innov_near, sems.at[sections]),
            pltpu.make_async_copy(damping, damping_near, sems.at[sections + 1]),
        ]
        copies = nearer + copies
    for copy in copies:
        copy.start()
    if relayed:
        for copy in nearer:
            copy.wait()
        obs = innov.shape[1]
        first = lax.axis_index("lev") * levels + (me ^ relayed) * chunk
        for k in range(chunk):
            relay[k : k + 1, obs:] = damping_near[pl.ds(first + k, 1), :]
        for piece in range(sections):

            @pl.when(me ^ relayed == piece)
            def _(here=slice(piece * chunk, (piece + 1) * chunk)):
                relay[:, 0:obs] = innov_near[here, :]

        copies = copies[2:]
    for copy in copies:
        copy.wait()


def cut_chunks(field, innov, damping, sections, relayed):
    levels, lats, lons = field.shape
    chunk = max(1, levels // sections)
    out_shape = [jax.ShapeDtypeStruct((chunk, lats, lons), jnp.float32)] * sections
    scratch = []
    if relayed:
        width = innov.shape[1] + damping.shape[1]
        out_shape = out_shape + [jax.ShapeDtypeStruct((chunk, width), jnp.float32)]
        scratch = [pltpu.VMEM(innov.shape, jnp.float32), pltpu.VMEM(damping.shape, jnp.float32)]
    return pl.pallas_call(
        functools.partial(cut_kernel, sections=sections, relayed=relayed),
        out_shape=out_shape,
        in_specs=[pl.BlockSpec(memory_space=pl.ANY)] * 3,
        out_specs=[vmem()] * len(out_shape),
        scratch_shapes=scratch + [pltpu.SemaphoreType.DMA((sections + 2,))],
        compiler_params=pltpu.CompilerParams(vmem_limit_bytes=6 * 2**20),
        name="cut",
    )(*in_hbm(field, innov, damping))


def scatter_scratch(levels, chunk, size, slots, sum_rows):
    return (
        [
            pltpu.VMEM((levels // chunk, size, LANES), jnp.float32),
            pltpu.SemaphoreType.DMA((slots,)),
            pltpu.VMEM((OBS_BLOCK, LANES), jnp.float32),
            pltpu.VMEM((OBS_BLOCK, LANES), jnp.float32),
        ]
        + [pltpu.SMEM((OBS_BLOCK,), jnp.int32)] * INDEX_BUFFERS
        + [pltpu.SemaphoreType.DMA((INDEX_BUFFERS,))]
        + [pltpu.VMEM((sum_rows, LANES), jnp.float32)] * ACCUMULATORS
    )


def forcing_chunks(cells, innov, damping, lats, lons, sections, slots):
    levels = innov.shape[0]
    span = LANES // levels
    rows = (cells // (lons * span)) * lons + cells % lons
    chunk = max(1, levels // sections)
    size = chunk * lats * lons // LANES + SUBLANES
    return pl.pallas_call(
        functools.partial(
            scatter_kernel,
            sections=sections,
            slots=slots,
            relayed=False,
            lats=lats,
            lons=lons,
        ),
        out_shape=[jax.ShapeDtypeStruct((size, LANES), jnp.float32)] * slots,
        in_specs=[pl.BlockSpec(memory_space=pl.ANY), vmem(), vmem(), vmem()],
        out_specs=[pl.BlockSpec(memory_space=pl.ANY)] * slots,
        scratch_shapes=scatter_scratch(levels, chunk, size, slots, lats * lons // span),
        compiler_params=pltpu.CompilerParams(vmem_limit_bytes=32 * 2**20),
        name="scatter",
    )(rows, *in_hbm(cells[None, :], innov, damping))


def sweep_kernel(analysis, synthesis, fourier, spread, *refs, sections):
    chunks, tangents = refs[:sections], refs[sections : 2 * sections]
    out, forced, work, filtered, total, damp_now = refs[2 * sections :]
    fourier_high, fourier_low = fourier.at[0], fourier.at[1]
    waves, lats = analysis.shape[:2]
    times = sections
    degree_block = waves // times
    kept = tangents[0].shape[0]
    lons = tangents[0].shape[2]
    levels = spread.shape[0] // lax.axis_size("lev")
    half = 2 * kept
    rows = max(SUBLANES, 2 * half)
    copies = rows // half
    row = lax.broadcasted_iota(jnp.int32, (rows, waves), 0)
    is_high = (row // half) % 2 == 0
    total[...] = jnp.zeros(total.shape, jnp.float32)
    forced[...] = jnp.zeros(forced.shape, jnp.float32)
    me = lax.axis_index("tm")

    for time in range(times - 1, -1, -1):
        for slot in range(sections):

            @pl.when(me ^ slot == time)
            def _(chunk=chunks[slot]):
                for k in range(kept):
                    here = slice(k * lats, (k + 1) * lats)
                    for west in range(lons // LANES):
                        there = slice(west * LANES, (west + 1) * LANES)
                        at = (k * (lons // LANES) + west) * lats
                        forced[here, there] = forced[here, there] + chunk[at : at + lats, :]
                    tail = kept * lats * lons // LANES + k
                    damp_now[k : k + 1, :] = chunk[tail : tail + 1, :]

        high, low = split_parts(forced[...])
        coeffs = dot(fourier_high[...], high, 1, 1)
        coeffs = coeffs + dot(fourier_low[...], high, 1, 1)
        coeffs = coeffs + dot(fourier_high[...], low, 1, 1)
        for k in range(kept):
            for p in range(2):
                piece = coeffs[p * waves : (p + 1) * waves, k * lats : (k + 1) * lats]
                piece_high = piece.astype(jnp.bfloat16).astype(jnp.float32)
                piece_low = piece - piece_high
                for copy in range(copies):
                    at = copy * half + 2 * k + p
                    work[pl.ds(at, waves, stride=rows), :] = (
                        piece_high if copy % 2 == 0 else piece_low
                    )
        damp_rows = []
        for k in range(kept):
            damp_row = damp_now[k : k + 1, :]
            damp_rows += [damp_row, damp_row]
        damp = jnp.concatenate(damp_rows * copies, axis=0)

        def analyse(group, carry):
            for step in range(WAVE_UNROLL):
                wave = group * WAVE_UNROLL + step
                at = pl.ds(pl.multiple_of(wave * rows, rows), rows)
                product = dot(work[at, :].astype(jnp.bfloat16), analysis[wave], 1, 0)
                product = product[:, 0:waves] + product[:, waves:]
                spectral = product + pltpu.roll(product, half, 0)
                total[at, :] = total[at, :] + spectral
                if time > 0:
                    damped = spectral * damp
                    part = damped.astype(jnp.bfloat16).astype(jnp.float32)
                    filtered[at, :] = jnp.where(is_high, part, damped - part)
            return carry

        def synthesise(group, carry):
            for step in range(WAVE_UNROLL):
                wave = group * WAVE_UNROLL + step
                at = pl.ds(pl.multiple_of(wave * rows, rows), rows)
                result = dot(filtered[at, :].astype(jnp.bfloat16), synthesis[wave], 1, 0)
                result = result[:, 0:lats] + result[:, lats:]
                work[at, :] = result + pltpu.roll(result, half, 0)
            return carry

        lax.fori_loop(0, waves // WAVE_UNROLL, analyse, 0)
        if time > 0:
            for slot in range(sections):

                @pl.when(me ^ slot == time)
                def _(factor=tangents[slot]):
                    for k in range(kept):
                        here = slice(k * lats, (k + 1) * lats)
                        forced[here, :] = factor[k] * forced[here, :]

            lax.fori_loop(0, waves // WAVE_UNROLL, synthesise, 0)
            for k in range(kept):
                parts = [work[pl.ds(2 * k + p, waves, stride=rows), :].T for p in range(2)]
                synth_high, synth_low = split_parts(jnp.concatenate(parts, axis=1))
                gridded = dot(synth_high, fourier_high[...], 1, 0)
                gridded = gridded + dot(synth_high, fourier_low[...], 1, 0)
                gridded = gridded + dot(synth_low, fourier_high[...], 1, 0)
                here = slice(k * lats, (k + 1) * lats)
                forced[here, :] = forced[here, :] + gridded

    scaled = []
    repeat = max(1, sections // levels)
    first = lax.axis_index("lev") * levels + (me // repeat) * kept
    for k in range(kept):
        factor = spread[pl.ds(first + k, 1), :]
        for p in range(2):
            scaled.append(total[pl.ds(2 * k + p, waves, stride=rows), :] * factor)
    for block in range(times):
        cols = slice(block * degree_block, (block + 1) * degree_block)
        out[block] = jnp.concatenate([piece[:, cols] for piece in scaled], axis=1)


def sweep(chunks, tangents, tables):
    sections = len(chunks)
    kept, lats, lons = tangents[0].shape
    waves = tables[0].shape[0]
    rows = max(SUBLANES, 4 * kept)
    return pl.pallas_call(
        functools.partial(sweep_kernel, sections=sections),
        out_shape=jax.ShapeDtypeStruct(
            (sections, waves, 2 * kept * waves // sections), jnp.float32
        ),
        in_specs=[vmem()] * (4 + 2 * sections),
        out_specs=vmem(),
        scratch_shapes=[
            pltpu.VMEM((kept * lats, lons), jnp.float32),
            pltpu.VMEM((waves * rows, lats), jnp.float32),
            pltpu.VMEM((waves * rows, waves), jnp.float32),
            pltpu.VMEM((waves * rows, waves), jnp.float32),
            pltpu.VMEM((SUBLANES, waves), jnp.float32),
        ],
        compiler_params=pltpu.CompilerParams(vmem_limit_bytes=SWEEP_MIB * 2**20),
        name="sweep",
    )(*tables, *chunks, *tangents)


def mix_kernel(owned, vertical, out, *, sections, groups, repeat):
    peers = sections * groups
    block_waves = owned.shape[0] // peers
    lanes = owned.shape[1]
    steps = sections // repeat
    levels = vertical.shape[0] // groups
    kept = levels // steps
    each = lanes // kept
    columns = []
    for wave in range(block_waves):
        pieces = [
            owned[pl.ds(step * repeat * groups * block_waves + wave, groups, stride=block_waves), :]
            for step in range(steps)
        ]
        columns.append(jnp.concatenate(pieces, axis=0))
    high, low = split_parts(jnp.concatenate(columns, axis=1))
    left = jnp.concatenate([high, low, high], axis=0)
    for k in range(kept):
        pieces = [
            vertical[pl.ds(step * kept + k, groups, stride=levels), :] for step in range(steps)
        ]
        mix_high, mix_low = split_parts(jnp.concatenate(pieces, axis=0))
        product = dot(left, jnp.concatenate([mix_high, mix_high, mix_low], axis=0), 0, 0)
        for wave in range(block_waves):
            start = wave * lanes + k * each
            piece = product[start : start + each, :]
            out[wave] = piece if k == 0 else out[wave] + piece


def mix(owned, vertical, sections, groups, repeat):
    peers, block_waves, lanes = owned.shape
    steps = sections // repeat
    each = lanes // (vertical.shape[0] // groups // steps)
    return pl.pallas_call(
        functools.partial(mix_kernel, sections=sections, groups=groups, repeat=repeat),
        out_shape=jax.ShapeDtypeStruct((block_waves, each, vertical.shape[1]), jnp.float32),
        in_specs=[vmem()] * 2,
        out_specs=vmem(),
        compiler_params=pltpu.CompilerParams(vmem_limit_bytes=16 * 2**20),
        name="mix",
    )(owned.reshape(peers * block_waves, lanes), vertical)


def shards(obs_cell, innovation, tangent, damping, spread, vertical):
    sections = lax.axis_size("tm")
    groups = lax.axis_size("lev")
    lev_dev, lat_rows, lon_cols = tangent.shape[1:]
    wave_count = damping.shape[2]
    repeat = max(1, sections // lev_dev)
    kept = max(1, lev_dev // sections)

    relayed = sections - 1 if lev_dev >= sections > 2 else 0
    direct = relayed or sections

    def send(value, slot):
        return lax.ppermute(value, "tm", [(i, i ^ slot) for i in range(sections)])

    def exchange(chunks):
        return [send(chunk, slot) if slot else chunk for slot, chunk in enumerate(chunks)]

    cells, innov, rates = obs_cell[0], innovation[0], damping[0]
    cut = cut_chunks(tangent[0], innov, rates, sections, relayed)
    if relayed:
        far = send(cut[sections], relayed)
        far_cells = send(obs_cell, relayed)[0]
    tangents = exchange(cut[:sections])
    chunks = forcing_chunks(
        cells, innov, rates, lat_rows, lon_cols, sections, direct
    )
    chunks = exchange(chunks)
    if relayed:
        chunk, tables = far_chunk_and_tables(
            far_cells, far, rates, lat_rows, lon_cols, wave_count, spread
        )
        chunks.append(chunk)
    else:
        tables = legendre_tables(lat_rows, lon_cols, wave_count, spread)
    blocks = sweep(chunks, tangents, tables)

    block_waves = wave_count // groups
    block_degrees = wave_count // sections
    blocks = blocks.reshape(sections * groups, block_waves, 2 * kept * block_degrees)
    owned = lax.all_to_all(blocks, ("tm", "lev"), split_axis=0, concat_axis=0, tiled=True)
    mixed = mix(owned, vertical, sections, groups, repeat)
    mixed = mixed.reshape(block_waves, 2, block_degrees, vertical.shape[1])
    return jnp.transpose(mixed, (3, 0, 1, 2))


def solution(mesh):
    placed = (
        P("tm", None),
        P("tm", "lev", None),
        P("tm", "lev", None, None),
        P("tm", None, None),
        P(),
        P(),
    )
    return jax.shard_map(
        shards, mesh=mesh, in_specs=placed, out_specs=P(None, "lev", None, "tm"), check_vma=False
    )
```

```python
import functools
import math

import numpy as np

import jax
import jax.numpy as jnp
from jax import lax
from jax.experimental import pallas as pl
from jax.experimental.pallas import tpu as pltpu
from jax.sharding import PartitionSpec as P


LANES = 128
SUBLANES = 8
ACCUMULATORS = 8
OBS_BLOCK = 1024
INDEX_BUFFERS = 4
WAVE_UNROLL = 64
DEGREE_BLOCK = 16
TABLE_UNROLL = 8
SWEEP_MIB = 20


def vmem():
    return pl.BlockSpec(memory_space=pltpu.VMEM)


def in_hbm(*arrays):
    return [pltpu.with_memory_space_constraint(array, pltpu.HBM) for array in arrays]


def fourier_rows(lon_count, wave_count):
    longitude = np.arange(lon_count)[None, :]
    wavenumber = np.arange(wave_count)[:, None]
    angles = (longitude * wavenumber % lon_count) * (2.0 * math.pi / lon_count)
    rows = np.concatenate([np.cos(angles), np.sin(angles)]) * math.sqrt(2.0 / lon_count)
    rows = rows.astype(np.float32)
    high = rows.astype(jnp.bfloat16)
    low = (rows - high.astype(np.float32)).astype(jnp.bfloat16)
    return high, low


def legendre_seeds(lat_count, wave_count):
    orders = np.arange(wave_count, dtype=np.float64)[:, None]
    degrees = np.arange(wave_count, dtype=np.float64)[None, :]
    latitude = (np.arange(lat_count) + 0.5) * (math.pi / lat_count) - 0.5 * math.pi
    sine = np.sin(latitude)[None, :]
    cosine = np.cos(latitude)[None, :]
    gammas = np.array(
        [
            math.lgamma(order + 1.5) - math.lgamma(1.5) - math.lgamma(order + 1.0)
            for order in range(wave_count)
        ]
    )[:, None]
    diagonal = np.exp(-0.5 * math.log(2.0) + 0.5 * gammas + orders * np.log(cosine))
    diagonal = diagonal * np.sqrt(math.pi / lat_count * cosine)
    upward = np.sqrt(
        np.maximum(4.0 * degrees**2 - 1.0, 1.0) / np.maximum(degrees**2 - orders**2, 1.0)
    )
    lower = degrees - 1.0
    downward = np.sqrt(
        np.maximum(lower**2 - orders**2, 0.0) / np.maximum(4.0 * lower**2 - 1.0, 1.0)
    )
    sine = np.broadcast_to(sine, (SUBLANES, lat_count))
    return np.concatenate([upward, upward * downward, diagonal, sine]).astype(np.float32)


def split_parts(values):
    high = values.astype(jnp.bfloat16)
    low = (values - high.astype(jnp.float32)).astype(jnp.bfloat16)
    return high, low


def dot(left, right, left_dim, right_dim):
    return lax.dot_general(
        left, right, (((left_dim,), (right_dim,)), ((), ())), preferred_element_type=jnp.float32
    )


def bring_near(fourier, spread, fourier_near, spread_near, sems):
    return [
        pltpu.make_async_copy(fourier, fourier_near, sems.at[0]),
        pltpu.make_async_copy(spread, spread_near, sems.at[1]),
    ]


def legendre_values(seeds, values):
    lats = values.shape[1]
    waves = seeds.shape[0] // 3 // DEGREE_BLOCK * DEGREE_BLOCK
    pitch = values.shape[0] // waves
    sine = seeds[3 * waves : 3 * waves + 1, :]
    one = jnp.zeros((0, lats), jnp.float32)
    two = one
    for degree in range(waves):
        live = (degree // DEGREE_BLOCK + 1) * DEGREE_BLOCK
        if one.shape[0] < live:
            fresh = jnp.zeros((live - one.shape[0], lats), jnp.float32)
            one = jnp.concatenate([one, fresh], axis=0) if one.shape[0] else fresh
            two = jnp.concatenate([two, fresh], axis=0) if two.shape[0] else fresh
        order = lax.broadcasted_iota(jnp.int32, (DEGREE_BLOCK, lats), 0) + (live - DEGREE_BLOCK)
        edge = slice(2 * waves + live - DEGREE_BLOCK, 2 * waves + live)
        seed = jnp.where(order == degree, seeds[edge, :], 0.0)
        if live > DEGREE_BLOCK:
            seed = jnp.concatenate(
                [jnp.zeros((live - DEGREE_BLOCK, lats), jnp.float32), seed], axis=0
            )
        up = seeds[0:live, degree : degree + 1]
        down = seeds[waves : waves + live, degree : degree + 1]
        current = (up * sine) * one - down * two + seed
        values[degree * pitch : degree * pitch + live, :] = current
        one, two = current, one


def write_tables(values, analysis, synthesis, wave, skipped, turn, lead=0):
    waves, lats = analysis.shape[:2]
    pitch = waves + SUBLANES
    start = (skipped + lead) * pitch + wave
    rows = values[pl.ds(start, waves - skipped, stride=pitch), :]
    if skipped:
        rows = jnp.concatenate([jnp.zeros((skipped, lats), jnp.float32), rows], axis=0)
    high, low = split_parts(rows)
    synthesis[wave] = jnp.concatenate([high, low], axis=1)
    if turn:
        row = lax.broadcasted_iota(jnp.int32, (lats, lats), 0)
        column = lax.broadcasted_iota(jnp.int32, (lats, lats), 1)
        identity = (row == column).astype(jnp.bfloat16)
        both = jnp.concatenate([high, low], axis=0)
        analysis[wave] = dot(identity, both, 1, 1).astype(jnp.bfloat16)
    else:
        analysis[wave] = jnp.concatenate(split_parts(rows.T), axis=1)


def legendre_kernel(
    seeds, fourier, spread, analysis, synthesis, fourier_near, spread_near, values, sems
):
    waves = analysis.shape[0]
    nearer = bring_near(fourier, spread, fourier_near, spread_near, sems)
    for copy in nearer:
        copy.start()
    legendre_values(seeds, values)
    for group in range(waves // DEGREE_BLOCK):
        skipped = group * DEGREE_BLOCK

        def emit(part, carry):
            for step in range(TABLE_UNROLL):
                wave = skipped + TABLE_UNROLL * part + step
                write_tables(values, analysis, synthesis, wave, skipped, step % 2)
            return carry

        lax.fori_loop(0, DEGREE_BLOCK // TABLE_UNROLL, emit, 0)
    for copy in nearer:
        copy.wait()


def near_kernel(rows, cells, innov, damping, seeds, *refs, sections, slots, lats, lons):
    values, seeds_near, up_now, down_now, sem = refs[slots : slots + 5]
    waves = up_now.shape[0]
    pitch = waves + SUBLANES
    each = waves // (cells.shape[1] // OBS_BLOCK)
    nearer = pltpu.make_async_copy(seeds, seeds_near, sem.at[0])
    nearer.start()
    values[0 : 2 * pitch, :] = jnp.zeros((2 * pitch, lats), jnp.float32)
    nearer.wait()
    up_now[...] = seeds_near[0:waves, :]
    down_now[...] = seeds_near[waves : 2 * waves, :]

    def some_degrees(block):
        order = lax.broadcasted_iota(jnp.int32, (waves, lats), 0)
        sine = seeds_near[3 * waves : 3 * waves + 1, :]

        def stored(degree):
            return pl.ds(pl.multiple_of((degree + 2) * pitch, SUBLANES), waves)

        one = values[stored(block * each - 1), :]
        two = values[stored(block * each - 2), :]
        for step in range(each):
            degree = block * each + step
            seed = jnp.where(order == degree, seeds_near[2 * waves : 3 * waves, :], 0.0)
            current = (up_now[:, step : step + 1] * sine) * one
            current = current - down_now[:, step : step + 1] * two + seed
            values[stored(degree), :] = current
            one, two = current, one
        up_now[...] = pltpu.roll(up_now[...], waves - each, 1)
        down_now[...] = pltpu.roll(down_now[...], waves - each, 1)

    scatter_kernel(
        rows,
        cells,
        innov,
        damping,
        *refs[:slots],
        *refs[slots + 5 :],
        sections=sections,
        slots=slots,
        relayed=False,
        lats=lats,
        lons=lons,
        beside=some_degrees,
    )


def near_chunks_and_values(cells, innov, damping, lats, lons, waves, sections, slots):
    levels = innov.shape[0]
    span = LANES // levels
    rows = (cells // (lons * span)) * lons + cells % lons
    chunk = max(1, levels // sections)
    size = chunk * lats * lons // LANES + SUBLANES
    seeds = legendre_seeds(lats, waves)
    anywhere = pl.BlockSpec(memory_space=pl.ANY)
    *chunks, values = pl.pallas_call(
        functools.partial(near_kernel, sections=sections, slots=slots, lats=lats, lons=lons),
        out_shape=[jax.ShapeDtypeStruct((size, LANES), jnp.float32)] * slots
        + [jax.ShapeDtypeStruct(((waves + 2) * (waves + SUBLANES), lats), jnp.float32)],
        in_specs=[anywhere, vmem(), vmem(), vmem(), anywhere],
        out_specs=[anywhere] * slots + [vmem()],
        scratch_shapes=[
            pltpu.VMEM(seeds.shape, jnp.float32),
            pltpu.VMEM((waves, waves), jnp.float32),
            pltpu.VMEM((waves, waves), jnp.float32),
            pltpu.SemaphoreType.DMA((1,)),
        ]
        + scatter_scratch(levels, chunk, size, slots, lats * lons // span),
        compiler_params=pltpu.CompilerParams(vmem_limit_bytes=32 * 2**20),
        name="near",
    )(rows, *in_hbm(cells[None, :], innov, damping, seeds))
    return chunks, values


def far_kernel(
    rows,
    cells,
    innov,
    damping,
    values,
    fourier,
    spread,
    chunk,
    analysis,
    synthesis,
    fourier_near,
    spread_near,
    near_sems,
    *scratch,
    lats,
    lons,
):
    nearer = bring_near(fourier, spread, fourier_near, spread_near, near_sems)
    for copy in nearer:
        copy.start()
    each = analysis.shape[0] // (cells.shape[1] // OBS_BLOCK)

    def some_tables(block):
        for step in range(each):
            write_tables(values, analysis, synthesis, block * each + step, 0, step % 2, 2)

    scatter_kernel(
        rows,
        cells,
        innov,
        damping,
        chunk,
        *scratch,
        sections=1,
        slots=1,
        relayed=True,
        lats=lats,
        lons=lons,
        beside=some_tables,
    )
    for copy in nearer:
        copy.wait()


def table_shapes(lats, waves, fourier, spread):
    return [
        jax.ShapeDtypeStruct((waves, lats, 2 * waves), jnp.bfloat16),
        jax.ShapeDtypeStruct((waves, waves, 2 * lats), jnp.bfloat16),
        jax.ShapeDtypeStruct(fourier.shape, jnp.bfloat16),
        jax.ShapeDtypeStruct(spread.shape, jnp.float32),
    ]


def far_chunk_and_tables(cells, innov, damping, values, lats, lons, waves, spread):
    levels = innov.shape[0]
    span = LANES // levels
    rows = (cells // (lons * span)) * lons + cells % lons
    size = levels * lats * lons // LANES + SUBLANES
    fourier = np.stack(fourier_rows(lons, waves))
    anywhere = pl.BlockSpec(memory_space=pl.ANY)
    far = [*in_hbm(damping), values, *in_hbm(fourier, spread)]
    chunk, *tables = pl.pallas_call(
        functools.partial(far_kernel, lats=lats, lons=lons),
        out_shape=[jax.ShapeDtypeStruct((size, LANES), jnp.float32)]
        + table_shapes(lats, waves, fourier, spread),
        in_specs=[anywhere, vmem(), vmem(), anywhere, vmem(), anywhere, anywhere],
        out_specs=[anywhere] + [vmem()] * 4,
        scratch_shapes=[pltpu.SemaphoreType.DMA((2,))]
        + scatter_scratch(levels, levels, size, 1, lats * lons // span),
        compiler_params=pltpu.CompilerParams(vmem_limit_bytes=14 * 2**20),
        name="far",
    )(rows, cells[None, :], innov, *far)
    return chunk, tables


def legendre_tables(lat_count, lon_count, wave_count, spread):
    pitch = wave_count + SUBLANES
    fourier = np.stack(fourier_rows(lon_count, wave_count))
    anywhere = pl.BlockSpec(memory_space=pl.ANY)
    return pl.pallas_call(
        legendre_kernel,
        out_shape=table_shapes(lat_count, wave_count, fourier, spread),
        in_specs=[vmem(), anywhere, anywhere],
        out_specs=[vmem()] * 4,
        scratch_shapes=[
            pltpu.VMEM((wave_count * pitch, lat_count), jnp.float32),
            pltpu.SemaphoreType.DMA((2,)),
        ],
        compiler_params=pltpu.CompilerParams(vmem_limit_bytes=14 * 2**20),
        name="legendre",
    )(*in_hbm(legendre_seeds(lat_count, wave_count), fourier, spread))


def scatter_kernel(
    rows, cells, innov, damping, *refs, sections, slots, relayed, lats, lons, beside=None
):
    levels = innov.shape[0]
    obs = cells.shape[1]
    outs, refs = refs[:slots], refs[slots:]
    field, sems = refs[:2]
    datas = refs[2:4]
    nears = refs[4 : 4 + INDEX_BUFFERS]
    near_sems = refs[4 + INDEX_BUFFERS]
    sums = refs[5 + INDEX_BUFFERS :]
    span = LANES // levels
    chunk = max(1, levels // sections)
    row = lax.broadcasted_iota(jnp.int32, (4 * SUBLANES, 2 * LANES), 0)
    lane = lax.broadcasted_iota(jnp.int32, (4 * SUBLANES, 2 * LANES), 1)
    values_here = (row < 3 * SUBLANES) & (lane < LANES) & (row % SUBLANES == lane // span)
    place = (values_here | ((row == 3 * SUBLANES) & (lane >= LANES))).astype(jnp.bfloat16)
    lane_low = (lax.broadcasted_iota(jnp.int32, (OBS_BLOCK, LANES), 1) % span).astype(jnp.float32)

    def spread_out(block, data):
        start = pl.multiple_of(block * OBS_BLOCK, OBS_BLOCK)
        rest = innov[:, pl.ds(start, OBS_BLOCK)]
        if levels < SUBLANES:
            fill = jnp.zeros((SUBLANES - levels, OBS_BLOCK), jnp.float32)
            rest = jnp.concatenate([rest, fill], axis=0)
        parts = []
        for _ in range(3):
            parts.append(rest.astype(jnp.bfloat16).astype(jnp.float32))
            rest = rest - parts[-1]
        low = (cells[:, pl.ds(start, OBS_BLOCK)] // lons % span).astype(jnp.float32)
        parts.append(jnp.broadcast_to(low, (SUBLANES, OBS_BLOCK)))
        stacked = jnp.concatenate(parts, axis=0).astype(jnp.bfloat16)
        placed = dot(stacked, place, 0, 0)
        data[...] = jnp.where(placed[:, LANES:] == lane_low, placed[:, :LANES], 0.0)

    def add_rows(near, data):
        for step in range(OBS_BLOCK):
            part = sums[step % ACCUMULATORS]
            at = pl.ds(near[step], 1)
            part[at, :] = part[at, :] + data[step : step + 1, :]

    def fetch(block, buffer):
        start = pl.multiple_of(block * OBS_BLOCK, OBS_BLOCK)
        return pltpu.make_async_copy(
            rows.at[pl.ds(start, OBS_BLOCK)], nears[buffer], near_sems.at[buffer]
        )

    blocks = obs // OBS_BLOCK
    for buffer in range(INDEX_BUFFERS):
        fetch(buffer, buffer).start()
    for part in sums:
        part[...] = jnp.zeros(part.shape, jnp.float32)
    spread_out(0, datas[0])

    def some_blocks(group, carry):
        for buffer in range(INDEX_BUFFERS):
            block = group * INDEX_BUFFERS + buffer
            fetch(block, buffer).wait()
            spread_out(jnp.minimum(block + 1, blocks - 1), datas[(buffer + 1) % 2])
            if beside:
                beside(block)
            add_rows(nears[buffer], datas[buffer % 2])

            @pl.when(block + INDEX_BUFFERS < blocks)
            def _():
                fetch(block + INDEX_BUFFERS, buffer).start()

        return carry

    lax.fori_loop(0, blocks // INDEX_BUFFERS, some_blocks, 0)

    first = lax.axis_index("lev") * levels
    for high in range(lats // span):
        for west in range(lons // LANES):
            block = pl.ds(high * lons + west * LANES, LANES)
            total = sums[0][block, :]
            for part in sums[1:]:
                total = total + part[block, :]
            turned = total.T
            for k in range(levels):
                at = ((k % chunk) * (lons // LANES) + west) * lats + high * span
                field[k // chunk, at : at + span, :] = turned[k * span : (k + 1) * span, :]
    tail = chunk * lats * lons // LANES
    for piece in range(levels // chunk):
        field[piece, tail:, :] = jnp.zeros((SUBLANES, LANES), jnp.float32)
        for k in range(chunk):
            if relayed:
                rates = innov[k : k + 1, obs:]
            else:
                rates = damping[pl.ds(first + piece * chunk + k, 1), :]
            field[piece, tail + k : tail + k + 1, :] = rates
    me = lax.axis_index("tm")
    repeat = max(1, sections // levels)
    pieces = levels // chunk
    copies = [
        pltpu.make_async_copy(field.at[(me ^ slot) // repeat % pieces], outs[slot], sems.at[slot])
        for slot in range(slots)
    ]
    for copy in copies:
        copy.start()
    for copy in copies:
        copy.wait()


def cut_kernel(field, innov, damping, *refs, sections, relayed):
    outs, refs = refs[:sections], refs[sections:]
    levels = field.shape[0]
    me = lax.axis_index("tm")
    chunk = max(1, levels // sections)
    repeat = max(1, sections // levels)
    sems = refs[-1]
    copies = [
        pltpu.make_async_copy(
            field.at[pl.ds(((me ^ slot) // repeat) * chunk, chunk)], outs[slot], sems.at[slot]
        )
        for slot in range(sections)
    ]
    if relayed:
        relay, innov_near, damping_near = refs[:3]
        nearer = [
            pltpu.make_async_copy(innov, innov_near, sems.at[sections]),
            pltpu.make_async_copy(damping, damping_near, sems.at[sections + 1]),
        ]
        copies = nearer + copies
    for copy in copies:
        copy.start()
    if relayed:
        for copy in nearer:
            copy.wait()
        obs = innov.shape[1]
        first = lax.axis_index("lev") * levels + (me ^ relayed) * chunk
        for k in range(chunk):
            relay[k : k + 1, obs:] = damping_near[pl.ds(first + k, 1), :]
        for piece in range(sections):

            @pl.when(me ^ relayed == piece)
            def _(here=slice(piece * chunk, (piece + 1) * chunk)):
                relay[:, 0:obs] = innov_near[here, :]

        copies = copies[2:]
    for copy in copies:
        copy.wait()


def cut_chunks(field, innov, damping, sections, relayed):
    levels, lats, lons = field.shape
    chunk = max(1, levels // sections)
    out_shape = [jax.ShapeDtypeStruct((chunk, lats, lons), jnp.float32)] * sections
    scratch = []
    if relayed:
        width = innov.shape[1] + damping.shape[1]
        out_shape = out_shape + [jax.ShapeDtypeStruct((chunk, width), jnp.float32)]
        scratch = [pltpu.VMEM(innov.shape, jnp.float32), pltpu.VMEM(damping.shape, jnp.float32)]
    return pl.pallas_call(
        functools.partial(cut_kernel, sections=sections, relayed=relayed),
        out_shape=out_shape,
        in_specs=[pl.BlockSpec(memory_space=pl.ANY)] * 3,
        out_specs=[vmem()] * len(out_shape),
        scratch_shapes=scratch + [pltpu.SemaphoreType.DMA((sections + 2,))],
        compiler_params=pltpu.CompilerParams(vmem_limit_bytes=6 * 2**20),
        name="cut",
    )(*in_hbm(field, innov, damping))


def scatter_scratch(levels, chunk, size, slots, sum_rows):
    return (
        [
            pltpu.VMEM((levels // chunk, size, LANES), jnp.float32),
            pltpu.SemaphoreType.DMA((slots,)),
            pltpu.VMEM((OBS_BLOCK, LANES), jnp.float32),
            pltpu.VMEM((OBS_BLOCK, LANES), jnp.float32),
        ]
        + [pltpu.SMEM((OBS_BLOCK,), jnp.int32)] * INDEX_BUFFERS
        + [pltpu.SemaphoreType.DMA((INDEX_BUFFERS,))]
        + [pltpu.VMEM((sum_rows, LANES), jnp.float32)] * ACCUMULATORS
    )


def forcing_chunks(cells, innov, damping, lats, lons, sections, slots):
    levels = innov.shape[0]
    span = LANES // levels
    rows = (cells // (lons * span)) * lons + cells % lons
    chunk = max(1, levels // sections)
    size = chunk * lats * lons // LANES + SUBLANES
    return pl.pallas_call(
        functools.partial(
            scatter_kernel,
            sections=sections,
            slots=slots,
            relayed=False,
            lats=lats,
            lons=lons,
        ),
        out_shape=[jax.ShapeDtypeStruct((size, LANES), jnp.float32)] * slots,
        in_specs=[pl.BlockSpec(memory_space=pl.ANY), vmem(), vmem(), vmem()],
        out_specs=[pl.BlockSpec(memory_space=pl.ANY)] * slots,
        scratch_shapes=scatter_scratch(levels, chunk, size, slots, lats * lons // span),
        compiler_params=pltpu.CompilerParams(vmem_limit_bytes=32 * 2**20),
        name="scatter",
    )(rows, *in_hbm(cells[None, :], innov, damping))


def sweep_kernel(analysis, synthesis, fourier, spread, *refs, sections):
    chunks, tangents = refs[:sections], refs[sections : 2 * sections]
    out, forced, work, filtered, total, damp_now = refs[2 * sections :]
    fourier_high, fourier_low = fourier.at[0], fourier.at[1]
    waves, lats = analysis.shape[:2]
    times = sections
    degree_block = waves // times
    kept = tangents[0].shape[0]
    lons = tangents[0].shape[2]
    levels = spread.shape[0] // lax.axis_size("lev")
    half = 2 * kept
    rows = max(SUBLANES, 2 * half)
    copies = rows // half
    row = lax.broadcasted_iota(jnp.int32, (rows, waves), 0)
    is_high = (row // half) % 2 == 0
    total[...] = jnp.zeros(total.shape, jnp.float32)
    forced[...] = jnp.zeros(forced.shape, jnp.float32)
    me = lax.axis_index("tm")

    for time in range(times - 1, -1, -1):
        for slot in range(sections):

            @pl.when(me ^ slot == time)
            def _(chunk=chunks[slot]):
                for k in range(kept):
                    here = slice(k * lats, (k + 1) * lats)
                    for west in range(lons // LANES):
                        there = slice(west * LANES, (west + 1) * LANES)
                        at = (k * (lons // LANES) + west) * lats
                        forced[here, there] = forced[here, there] + chunk[at : at + lats, :]
                    tail = kept * lats * lons // LANES + k
                    damp_now[k : k + 1, :] = chunk[tail : tail + 1, :]

        high, low = split_parts(forced[...])
        coeffs = dot(fourier_high[...], high, 1, 1)
        coeffs = coeffs + dot(fourier_low[...], high, 1, 1)
        coeffs = coeffs + dot(fourier_high[...], low, 1, 1)
        for k in range(kept):
            for p in range(2):
                piece = coeffs[p * waves : (p + 1) * waves, k * lats : (k + 1) * lats]
                piece_high = piece.astype(jnp.bfloat16).astype(jnp.float32)
                piece_low = piece - piece_high
                for copy in range(copies):
                    at = copy * half + 2 * k + p
                    work[pl.ds(at, waves, stride=rows), :] = (
                        piece_high if copy % 2 == 0 else piece_low
                    )
        damp_rows = []
        for k in range(kept):
            damp_row = damp_now[k : k + 1, :]
            damp_rows += [damp_row, damp_row]
        damp = jnp.concatenate(damp_rows * copies, axis=0)

        def analyse(group, carry):
            for step in range(WAVE_UNROLL):
                wave = group * WAVE_UNROLL + step
                at = pl.ds(pl.multiple_of(wave * rows, rows), rows)
                product = dot(work[at, :].astype(jnp.bfloat16), analysis[wave], 1, 0)
                product = product[:, 0:waves] + product[:, waves:]
                spectral = product + pltpu.roll(product, half, 0)
                total[at, :] = total[at, :] + spectral
                if time > 0:
                    damped = spectral * damp
                    part = damped.astype(jnp.bfloat16).astype(jnp.float32)
                    filtered[at, :] = jnp.where(is_high, part, damped - part)
            return carry

        def synthesise(group, carry):
            for step in range(WAVE_UNROLL):
                wave = group * WAVE_UNROLL + step
                at = pl.ds(pl.multiple_of(wave * rows, rows), rows)
                result = dot(filtered[at, :].astype(jnp.bfloat16), synthesis[wave], 1, 0)
                result = result[:, 0:lats] + result[:, lats:]
                work[at, :] = result + pltpu.roll(result, half, 0)
            return carry

        lax.fori_loop(0, waves // WAVE_UNROLL, analyse, 0)
        if time > 0:
            for slot in range(sections):

                @pl.when(me ^ slot == time)
                def _(factor=tangents[slot]):
                    for k in range(kept):
                        here = slice(k * lats, (k + 1) * lats)
                        forced[here, :] = factor[k] * forced[here, :]

            lax.fori_loop(0, waves // WAVE_UNROLL, synthesise, 0)
            for k in range(kept):
                parts = [work[pl.ds(2 * k + p, waves, stride=rows), :].T for p in range(2)]
                synth_high, synth_low = split_parts(jnp.concatenate(parts, axis=1))
                gridded = dot(synth_high, fourier_high[...], 1, 0)
                gridded = gridded + dot(synth_high, fourier_low[...], 1, 0)
                gridded = gridded + dot(synth_low, fourier_high[...], 1, 0)
                here = slice(k * lats, (k + 1) * lats)
                forced[here, :] = forced[here, :] + gridded

    scaled = []
    repeat = max(1, sections // levels)
    first = lax.axis_index("lev") * levels + (me // repeat) * kept
    for k in range(kept):
        factor = spread[pl.ds(first + k, 1), :]
        for p in range(2):
            scaled.append(total[pl.ds(2 * k + p, waves, stride=rows), :] * factor)
    for block in range(times):
        cols = slice(block * degree_block, (block + 1) * degree_block)
        out[block] = jnp.concatenate([piece[:, cols] for piece in scaled], axis=1)


def sweep(chunks, tangents, tables):
    sections = len(chunks)
    kept, lats, lons = tangents[0].shape
    waves = tables[0].shape[0]
    rows = max(SUBLANES, 4 * kept)
    return pl.pallas_call(
        functools.partial(sweep_kernel, sections=sections),
        out_shape=jax.ShapeDtypeStruct(
            (sections, waves, 2 * kept * waves // sections), jnp.float32
        ),
        in_specs=[vmem()] * (4 + 2 * sections),
        out_specs=vmem(),
        scratch_shapes=[
            pltpu.VMEM((kept * lats, lons), jnp.float32),
            pltpu.VMEM((waves * rows, lats), jnp.float32),
            pltpu.VMEM((waves * rows, waves), jnp.float32),
            pltpu.VMEM((waves * rows, waves), jnp.float32),
            pltpu.VMEM((SUBLANES, waves), jnp.float32),
        ],
        compiler_params=pltpu.CompilerParams(vmem_limit_bytes=SWEEP_MIB * 2**20),
        name="sweep",
    )(*tables, *chunks, *tangents)


def mix_kernel(owned, vertical, out, *, sections, groups, repeat):
    peers = sections * groups
    block_waves = owned.shape[0] // peers
    lanes = owned.shape[1]
    steps = sections // repeat
    levels = vertical.shape[0] // groups
    kept = levels // steps
    each = lanes // kept
    columns = []
    for wave in range(block_waves):
        pieces = [
            owned[pl.ds(step * repeat * groups * block_waves + wave, groups, stride=block_waves), :]
            for step in range(steps)
        ]
        columns.append(jnp.concatenate(pieces, axis=0))
    high, low = split_parts(jnp.concatenate(columns, axis=1))
    left = jnp.concatenate([high, low, high], axis=0)
    for k in range(kept):
        pieces = [
            vertical[pl.ds(step * kept + k, groups, stride=levels), :] for step in range(steps)
        ]
        mix_high, mix_low = split_parts(jnp.concatenate(pieces, axis=0))
        product = dot(left, jnp.concatenate([mix_high, mix_high, mix_low], axis=0), 0, 0)
        for wave in range(block_waves):
            start = wave * lanes + k * each
            piece = product[start : start + each, :]
            out[wave] = piece if k == 0 else out[wave] + piece


def mix(owned, vertical, sections, groups, repeat):
    peers, block_waves, lanes = owned.shape
    steps = sections // repeat
    each = lanes // (vertical.shape[0] // groups // steps)
    return pl.pallas_call(
        functools.partial(mix_kernel, sections=sections, groups=groups, repeat=repeat),
        out_shape=jax.ShapeDtypeStruct((block_waves, each, vertical.shape[1]), jnp.float32),
        in_specs=[vmem()] * 2,
        out_specs=vmem(),
        compiler_params=pltpu.CompilerParams(vmem_limit_bytes=16 * 2**20),
        name="mix",
    )(owned.reshape(peers * block_waves, lanes), vertical)


def shards(obs_cell, innovation, tangent, damping, spread, vertical):
    sections = lax.axis_size("tm")
    groups = lax.axis_size("lev")
    lev_dev, lat_rows, lon_cols = tangent.shape[1:]
    wave_count = damping.shape[2]
    repeat = max(1, sections // lev_dev)
    kept = max(1, lev_dev // sections)

    relayed = sections - 1 if lev_dev >= sections > 2 else 0
    direct = relayed or sections

    def send(value, slot):
        return lax.ppermute(value, "tm", [(i, i ^ slot) for i in range(sections)])

    def exchange(chunks):
        return [send(chunk, slot) if slot else chunk for slot, chunk in enumerate(chunks)]

    cells, innov, rates = obs_cell[0], innovation[0], damping[0]
    cut = cut_chunks(tangent[0], innov, rates, sections, relayed)
    if relayed:
        *cut, cells_late = lax.optimization_barrier((*cut, obs_cell))
        far = send(cut[sections], relayed)
        far_cells = send(cells_late, relayed)[0]
    tangents = exchange(cut[:sections])
    if relayed:
        chunks, values = near_chunks_and_values(
            cells, innov, rates, lat_rows, lon_cols, wave_count, sections, direct
        )
    else:
        chunks = forcing_chunks(
            cells, innov, rates, lat_rows, lon_cols, sections, direct
        )
    chunks = exchange(chunks)
    if relayed:
        chunk, tables = far_chunk_and_tables(
            far_cells, far, rates, values, lat_rows, lon_cols, wave_count, spread
        )
        chunks.append(chunk)
    else:
        tables = legendre_tables(lat_rows, lon_cols, wave_count, spread)
    blocks = sweep(chunks, tangents, tables)

    block_waves = wave_count // groups
    block_degrees = wave_count // sections
    blocks = blocks.reshape(sections * groups, block_waves, 2 * kept * block_degrees)
    owned = lax.all_to_all(blocks, ("tm", "lev"), split_axis=0, concat_axis=0, tiled=True)
    mixed = mix(owned, vertical, sections, groups, repeat)
    mixed = mixed.reshape(block_waves, 2, block_degrees, vertical.shape[1])
    return jnp.transpose(mixed, (3, 0, 1, 2))


def solution(mesh):
    placed = (
        P("tm", None),
        P("tm", "lev", None),
        P("tm", "lev", None, None),
        P("tm", None, None),
        P(),
        P(),
    )
    return jax.shard_map(
        shards, mesh=mesh, in_specs=placed, out_specs=P(None, "lev", None, "tm"), check_vma=False
    )
```
